32 devices in a mesh: gz: 2 (over z_hi), gy: 4 (over z_lo, core), gx: 4 (over y, x).
Axes of the slice: x: 2, y: 2, z: 4 (z_hi: 2, z_lo: 2; z = z_hi * 2 + z_lo), core: 2. Of those that a mesh axis runs over, the one named last changes fastest.
Arguments:
- charges: float32 [65536], P(('gz', 'gy', 'gx')), may hold values from -2.5 to 2.5
- fractions: float32 [3, 65536], P(None, ('gz', 'gy', 'gx')), may hold values from 0 to 1
- base_cells: int32 [3, 65536], P(None, ('gz', 'gy', 'gx')), may hold values from 0 to 255, as said below
- counts: int32 [2, 4, 4], P('gz', 'gy', 'gx'), may hold values from 1024 to 2048, as said below
Outputs:
- forces: float32 [3, 65536], P(None, ('gz', 'gy', 'gx'))
The draws below stay inside these ranges and needn't reach their ends.
Inputs may be any that keep to these rules, and one draw needn't show every extreme that they name: `base_cells`: atom slots of the block at gz, gy, gx have base cells inside that block's cells: x in gx*64 to gx*64 + 63, y in gy*64 to gy*64 + 63, z in gz*128 to gz*128 + 127. The first counts[b] slots of block b hold atoms, the rest are empty; some block is full in every draw.
All inputs are finite; a program needn't handle non-finite values.
Results may differ from the reference program's by a relative error of at most 0.0003.
Values sent between devices are 32-bit elements; how exact they have to be, the bound alone decides.
A program may use at most 256 MiB of HBM per device.

```python
import jax
import jax.numpy as jnp

GRID = 256
ORDER = 4
CAP = 2048
CX = 64
CY = 64
CZ = 128
ATOMS = 65536


def draw_base_cells(key, part):
    blocks_x = GRID // CX
    blocks_y = GRID // CY
    blocks_z = GRID // CZ
    slot_index = jnp.arange(CAP * blocks_x * blocks_y * blocks_z, dtype=jnp.int32)
    block = slot_index // CAP
    block_x = block % blocks_x
    block_y = block // blocks_x % blocks_y
    block_z = block // (blocks_x * blocks_y)
    base_key = jax.random.fold_in(key, 11)
    key_x = jax.random.fold_in(base_key, 1)
    key_y = jax.random.fold_in(base_key, 2)
    key_z = jax.random.fold_in(base_key, 3)
    cell_x = block_x * CX + jax.random.randint(key_x, slot_index.shape, 0, CX, dtype=jnp.int32)
    cell_y = block_y * CY + jax.random.randint(key_y, slot_index.shape, 0, CY, dtype=jnp.int32)
    cell_z = block_z * CZ + jax.random.randint(key_z, slot_index.shape, 0, CZ, dtype=jnp.int32)
    return jnp.stack([cell_x, cell_y, cell_z]).astype(jnp.int32)


def draw_counts(key, part):
    blocks_x = GRID // CX
    blocks_y = GRID // CY
    blocks_z = GRID // CZ
    total = blocks_x * blocks_y * blocks_z
    base_key = jax.random.fold_in(key, 23)
    values = jax.random.randint(jax.random.fold_in(base_key, 1), (total,), CAP // 2, CAP + 1, dtype=jnp.int32)
    chosen = jax.random.randint(jax.random.fold_in(base_key, 2), (), 0, total, dtype=jnp.int32)
    values = jnp.where(jnp.arange(total, dtype=jnp.int32) == chosen, CAP, values)
    return values.reshape(blocks_z, blocks_y, blocks_x).astype(jnp.int32)


def block_levels(rng, dims, pieces, smallest, high):
    loudness, own = 1.0, jax.random.fold_in(rng, 6)
    for dim, blocks in pieces:
        heights = jnp.exp(jax.random.uniform(jax.random.fold_in(own, dim), (blocks,), jnp.float32, smallest / len(pieces), high / len(pieces)))
        loudness = loudness * jnp.repeat(heights, dims[dim] // blocks).reshape([-1 if axis == dim else 1 for axis in range(len(dims))])
    return loudness


def gaussian(key, shape, deviation, bound, split=(), held_as=jnp.bfloat16):
    loudness = block_levels(key, shape, split, -0.22, 0.18) if split else 1.0
    values = jax.random.normal(key, shape, jnp.float32) * deviation * loudness
    return jnp.minimum(jnp.maximum(values, -bound), bound).astype(held_as)


def setup_inputs(seed: int = 0) -> dict:
    splits = jax.random.split(jax.random.key(seed), 5)
    return {
        "charges": gaussian(splits[0], (ATOMS,), 0.4, 2.5, ((0, 32),), jnp.float32),
        "fractions": jnp.clip(1.0 * jax.random.uniform(splits[1], (3, ATOMS), jnp.float32) ** block_levels(splits[1], (3, ATOMS), ((1, 32),), -0.2, 0.2), 0.0, 1.0),
        "base_cells": draw_base_cells(jax.random.fold_in(splits[4], 71), 0),
        "counts": draw_counts(jax.random.fold_in(splits[4], 71), 0),
    }


coulomb = 332.0636
ewald = 0.7


def spline_weights(frac):
    rest = 1.0 - frac
    square = frac * frac
    cube = square * frac
    weights = jnp.stack([rest * rest * rest / 6.0, (3.0 * cube - 6.0 * square + 4.0) / 6.0,
                         (-3.0 * cube + 3.0 * square + 3.0 * frac + 1.0) / 6.0, cube / 6.0])
    slopes = jnp.stack([-0.5 * rest * rest, 1.5 * square - 2.0 * frac,
                        -1.5 * square + frac + 0.5, 0.5 * square])
    return weights, slopes


def green_factors(index, length):
    signed = jnp.where(2 * index < length, index, index - length).astype(jnp.float32)
    bspline = 36.0 / (4.0 + 2.0 * jnp.cos(index.astype(jnp.float32) * (2.0 * jnp.pi / length))) ** 2
    bspline = jnp.where(2 * index == length, 0.0, bspline)
    return signed * signed, bspline


def reference(charges, fractions, base_cells, counts):
    slot_index = jnp.arange(charges.shape[0], dtype=jnp.int32)
    live = (slot_index % CAP) < counts.reshape(-1)[slot_index // CAP]
    charge = jnp.where(live, charges, jnp.zeros_like(charges))
    weights_x, slopes_x = spline_weights(fractions[0])
    weights_y, slopes_y = spline_weights(fractions[1])
    weights_z, slopes_z = spline_weights(fractions[2])
    charge_grid = jnp.zeros((GRID, GRID, GRID), jnp.float32)
    for first in range(ORDER):
        for second in range(ORDER):
            for third in range(ORDER):
                cell_x = (base_cells[0] + first) % GRID
                cell_y = (base_cells[1] + second) % GRID
                cell_z = (base_cells[2] + third) % GRID
                charge_grid = charge_grid.at[cell_x, cell_y, cell_z].add(
                    charge * weights_x[first] * weights_y[second] * weights_z[third])
    index = jnp.arange(GRID, dtype=jnp.int32)
    square_line, spline_line = green_factors(index, GRID)
    square = square_line[:, None, None] + square_line[None, :, None] + square_line[None, None, :]
    factor = spline_line[:, None, None] * spline_line[None, :, None] * spline_line[None, None, :]
    green = jnp.where(square > 0.0,
                      coulomb * jnp.exp(square * (-(jnp.pi ** 2) / (ewald * ewald * GRID * GRID))) * factor
                      / (jnp.pi * GRID * jnp.maximum(square, 1.0)), 0.0)
    spectrum = jnp.fft.fftn(charge_grid)
    potential = jnp.real(jnp.fft.ifftn(spectrum * green)) * (GRID ** 3)
    force_x = jnp.zeros_like(charge)
    force_y = jnp.zeros_like(charge)
    force_z = jnp.zeros_like(charge)
    for first in range(ORDER):
        for second in range(ORDER):
            for third in range(ORDER):
                cell_x = (base_cells[0] + first) % GRID
                cell_y = (base_cells[1] + second) % GRID
                cell_z = (base_cells[2] + third) % GRID
                value = potential[cell_x, cell_y, cell_z]
                force_x = force_x + slopes_x[first] * weights_y[second] * weights_z[third] * value
                force_y = force_y + weights_x[first] * slopes_y[second] * weights_z[third] * value
                force_z = force_z + weights_x[first] * weights_y[second] * slopes_z[third] * value
    return -charge[None, :] * jnp.stack([force_x, force_y, force_z])
```

```python
import functools

import jax
import jax.numpy as jnp
import numpy as np
from jax import lax
from jax.experimental import pallas as pl
from jax.experimental.pallas import tpu as pltpu
from jax.sharding import PartitionSpec as P

GRID = 256
ORDER = 4
LANES = 128
SUBLANES = 8

coulomb = 332.0636
ewald = 0.7
MESH = pl.DeviceIdType.MESH
ROWS_BY_ROWS = (((1,), (1,)), ((), ()))


def round_up(value, unit):
    return -(-value // unit) * unit


def halves(value):
    high = value.astype(jnp.bfloat16)
    low = (value - high.astype(jnp.float32)).astype(jnp.bfloat16)
    return high, low


def constant_halves(value):
    value = np.asarray(value, np.float32)
    high = value.astype(jnp.bfloat16)
    low = (value - high.astype(np.float32)).astype(jnp.bfloat16)
    return jnp.asarray(np.stack([high, low]))


def mm(a, b, contract=(((1,), (0,)), ((), ()))):
    return lax.dot_general(a, b, contract, preferred_element_type=jnp.float32)


class Plan:
    def __init__(self, nz, ny, nx, capacity):
        self.nz, self.ny, self.nx = nz, ny, nx
        self.capacity = capacity
        self.chunks = capacity // LANES
        self.blocks = nz * nx
        self.cells_x = GRID // nx
        self.cells_y = GRID // ny
        self.cells_z = GRID // nz
        self.halo = ORDER - 1
        self.span_x = self.cells_x + self.halo
        self.span_y = self.cells_y + self.halo
        self.window = self.cells_z // nx
        self.octets = self.window // SUBLANES
        self.tiles = -(-self.span_y // nx)
        self.pad_y = self.tiles * nx
        self.rows = self.pad_y * SUBLANES
        self.dests = ny * nx
        self.kept = GRID // 2
        self.width_k = self.kept // self.dests
        self.pad_k = round_up(self.width_k, SUBLANES)
        self.row_k = 2 * self.pad_k
        self.all_y = ny * self.pad_y
        self.pad_x = round_up(self.span_x, SUBLANES)
        self.pack_x = round_up(3 * self.pad_x, LANES)
        assert nz == 2 and self.cells_z == LANES and self.span_x <= LANES

    def angle(self, outputs, inputs):
        return (outputs[:, None] * inputs[None, :] % GRID) * (2.0 * np.pi / GRID)

    def index_kx(self):
        place = np.arange(self.pad_k)
        index = np.arange(self.dests)[:, None] * self.width_k + np.minimum(place, self.width_k - 1)[None, :]
        return index.reshape(-1), np.tile(place < self.width_k, self.dests)

    def pairs(self, cosine, sine):
        shape = (self.dests, 1, self.pad_k, -1)
        both = np.concatenate([cosine.reshape(shape), sine.reshape(shape)], axis=1)
        return both.reshape(self.dests * self.row_k, -1)

    def x_forward(self):
        local = np.arange(LANES)
        cells = (np.arange(self.nx)[:, None] * self.cells_x + local[None, :]).reshape(-1)
        used = np.tile(local < self.span_x, self.nx)
        index, kept = self.index_kx()
        angle = self.angle(index, cells)
        mask = kept[:, None] * used[None, :]
        return constant_halves(self.pairs(np.cos(angle) * mask, -np.sin(angle) * mask))

    def x_inverse(self):
        lane = np.arange(self.pack_x)
        local = lane % self.pad_x
        cells = (np.arange(self.nx)[:, None] * self.cells_x + local[None, :]).reshape(-1)
        used = np.tile((local < self.span_x) & (lane < 3 * self.pad_x), self.nx)
        index, kept = self.index_kx()
        angle = self.angle(index, cells)
        mask = (kept * np.where(index > 0, 2.0, 1.0))[:, None] * used[None, :]
        return constant_halves(self.pairs(np.cos(angle) * mask, -np.sin(angle) * mask))

    def z_tables(self):
        cells = np.arange(self.cells_z)
        tables = []
        for parity in range(self.nz):
            angle = self.angle(self.nz * cells + parity, cells)
            forward = np.concatenate([np.cos(angle).T, np.sin(angle).T], axis=1)
            inverse = np.concatenate([np.cos(angle), np.sin(angle)], axis=1)
            tables += [constant_halves(forward), constant_halves(inverse)]
        return jnp.stack(tables).reshape(self.nz, 2, 2, self.cells_z, 2 * self.cells_z)

    def y_tables(self):
        local = np.arange(self.pad_y)
        cells = (np.arange(self.ny)[:, None] * self.cells_y + local[None, :]).reshape(-1)
        used = np.tile(local < self.span_y, self.ny)
        angle = self.angle(np.arange(GRID), cells)
        cosine, sine = np.cos(angle) * used[None, :], np.sin(angle) * used[None, :]
        forward = constant_halves(np.concatenate([cosine, sine], axis=1))
        inverse = constant_halves(np.concatenate([cosine.T, sine.T], axis=1))
        return forward, inverse

    def green_lines(self):
        index = np.arange(GRID)
        signed = np.where(2 * index < GRID, index, index - GRID)
        square = (signed * signed).astype(np.float32)
        bspline = 36.0 / (4.0 + 2.0 * np.cos(index * (2.0 * np.pi / GRID))) ** 2
        bspline = np.where(2 * index == GRID, 0.0, bspline).astype(np.float32)
        line_x = np.stack([square, bspline])[:, : self.kept]
        line_y = np.stack([square, bspline])[:, :, None]
        line_z = np.stack([square, bspline]).reshape(2, 1, self.cells_z, self.nz)
        line_z = line_z.transpose(3, 0, 1, 2)
        return jnp.asarray(line_x), jnp.asarray(line_y), jnp.asarray(line_z)


def exchange_kernel(axes, sizes, same, src_ref, out_ref, send_sems, recv_sems, local_sem):
    count = int(np.prod(sizes))
    me = 0
    for axis, size in zip(axes, sizes):
        me = me * size + lax.axis_index(axis)

    def place(member):
        where = {}
        for axis, size in reversed(list(zip(axes, sizes))):
            where[axis] = lax.rem(member, size)
            member = member // size
        return where

    barrier = pltpu.get_barrier_semaphore()
    for step in range(1, count):
        pl.semaphore_signal(
            barrier, inc=1, device_id=place(lax.rem(me + step, count)), device_id_type=MESH
        )
    pl.semaphore_wait(barrier, count - 1)
    copies = []
    for step in range(1, count):
        peer = lax.rem(me + step, count)
        copy = pltpu.make_async_remote_copy(
            src_ref=src_ref if same else src_ref.at[peer],
            dst_ref=out_ref.at[me],
            send_sem=send_sems.at[step],
            recv_sem=recv_sems.at[step],
            device_id=place(peer),
            device_id_type=MESH,
        )
        copy.start()
        copies.append(copy)
    own = pltpu.make_async_copy(src_ref if same else src_ref.at[me], out_ref.at[me], local_sem)
    own.start()
    own.wait()
    for copy in copies:
        copy.wait()


def exchange(data, axes, collective_id, same=False):
    sizes = [lax.axis_size(axis) for axis in axes]
    count = int(np.prod(sizes))
    shape = ((count,) if same else ()) + data.shape
    return pl.pallas_call(
        functools.partial(exchange_kernel, axes, sizes, same),
        in_specs=[pl.BlockSpec(memory_space=pltpu.VMEM)],
        out_specs=pl.BlockSpec(memory_space=pltpu.VMEM),
        out_shape=jax.ShapeDtypeStruct(shape, data.dtype),
        scratch_shapes=[
            pltpu.SemaphoreType.DMA((count,)),
            pltpu.SemaphoreType.DMA((count,)),
            pltpu.SemaphoreType.DMA,
        ],
        compiler_params=pltpu.CompilerParams(
            collective_id=collective_id, has_side_effects=True
        ),
    )(data)


def spline_rows(frac):
    rest = 1.0 - frac
    square = frac * frac
    cube = square * frac
    weights = [
        rest * rest * rest / 6.0,
        (3.0 * cube - 6.0 * square + 4.0) / 6.0,
        (-3.0 * cube + 3.0 * square + 3.0 * frac + 1.0) / 6.0,
        cube / 6.0,
    ]
    slopes = [
        -0.5 * rest * rest,
        1.5 * square - 2.0 * frac,
        -1.5 * square + frac + 0.5,
        0.5 * square,
    ]
    return weights, slopes


def placed(offset, values, dim):
    total = jnp.zeros(offset.shape, jnp.float32)
    for k in range(ORDER):
        total = jnp.where(offset == float(k), values[k][dim : dim + 1], total)
    return total


def offsets(rows, lowest):
    return lax.broadcasted_iota(jnp.int32, (rows, LANES), 0).astype(jnp.float32) - lowest


def fold_sign(parity, part):
    return (1 - 2 * lax.rem(parity * part, 2)).astype(jnp.float32)


def over_chunks(plan, bounds_ref, work):
    first = lax.axis_index("gx") * plan.window

    def step(i, carry):
        low = bounds_ref[0, i]
        high = bounds_ref[1, i] + plan.halo

        def meets(start, length):
            inside = (low <= start + length - 1) & (high >= start)
            return inside | (high >= plan.cells_z + start)

        @pl.when(meets(first, plan.window))
        def _():
            work(i // plan.chunks, lax.rem(i, plan.chunks), meets)

        return carry

    lax.fori_loop(0, plan.blocks * plan.chunks, step, 0)


def z_rows(plan, values, lowest, parity):
    offset = offsets(plan.window, lowest - (lax.axis_index("gx") * plan.window).astype(jnp.float32))
    wrapped = placed(offset + float(plan.cells_z), values, 2)
    return placed(offset, values, 2) + fold_sign(parity, 1) * wrapped


def spread_kernel(plan, bounds_ref, atoms_ref, dft_ref, out_ref, grid_ref, y_ref, z_ref, x_ref, a_ref):
    parity = lax.axis_index("gz")
    first = lax.axis_index("gx") * plan.window
    grid_ref[...] = jnp.zeros_like(grid_ref)
    x_ref[...] = jnp.zeros_like(x_ref)

    def work(block, chunk, meets):
        atoms = atoms_ref[block, :, pl.ds(pl.multiple_of(chunk * LANES, LANES), LANES)]
        weights, _ = spline_rows(atoms[0:3])
        sign = fold_sign(parity, block // plan.nx)
        rows_x = placed(offsets(plan.pad_x, atoms[4:5]), weights, 0)
        y_ref[...] = placed(offsets(plan.pad_y, atoms[5:6]), weights, 1)
        z_ref[...] = z_rows(plan, weights, atoms[6:7], parity) * (atoms[3:4] * sign)
        rows_x = jnp.concatenate(
            [rows_x, jnp.zeros((LANES - plan.pad_x, LANES), jnp.float32)], axis=0
        )
        high, low = halves(rows_x)
        x_ref[:LANES, :LANES] = high
        x_ref[:LANES, LANES:] = high
        x_ref[LANES:, :LANES] = low
        place = pl.multiple_of(lax.rem(block, plan.nx) * LANES, LANES)
        for octet in range(plan.octets):

            @pl.when(meets(first + octet * SUBLANES, SUBLANES))
            def _():
                line = z_ref[octet * SUBLANES : (octet + 1) * SUBLANES]
                for y in range(0, plan.pad_y, 2):
                    pair = jnp.concatenate([y_ref[y : y + 1] * line, y_ref[y + 1 : y + 2] * line], axis=0)
                    high, low = halves(pair)
                    a_ref[y * SUBLANES : (y + 2) * SUBLANES, :LANES] = high
                    a_ref[y * SUBLANES : (y + 2) * SUBLANES, LANES:] = low
                product = mm(a_ref[...], x_ref[...], ROWS_BY_ROWS)
                grid_ref[octet, :, pl.ds(place, LANES)] += product[:, :LANES] + product[:, LANES:]

    over_chunks(plan, bounds_ref, work)

    def transform(tile, carry):
        pieces = []
        for part in range(plan.nx):
            row = pl.multiple_of((tile * plan.nx + part) * SUBLANES, SUBLANES)
            for octet in range(plan.octets):
                pieces.append(grid_ref[octet, pl.ds(row, SUBLANES), :])
        high, low = halves(jnp.concatenate(pieces, axis=0))
        first_pass = mm(dft_ref[0], jnp.concatenate([high, low], axis=0), ROWS_BY_ROWS)
        second_pass = mm(dft_ref[1], high, ROWS_BY_ROWS)
        total = first_pass[:, :LANES] + (first_pass[:, LANES:] + second_pass)
        here = pl.ds(pl.multiple_of(tile * LANES, LANES), LANES)
        out_ref[:, :, here] = total.reshape(plan.dests, plan.row_k, LANES)
        return carry

    lax.fori_loop(0, plan.tiles, transform, 0)


def regroup(plan, values):
    shape = values[0].shape
    group = lax.broadcasted_iota(jnp.int32, shape, 1) // plan.window
    moved = []
    for step in range(plan.nx):
        mixed = values[step % plan.nx]
        for part in range(1, plan.nx):
            mixed = jnp.where(group == part, values[(part + step) % plan.nx], mixed)
        moved.append(pltpu.roll(mixed, step * plan.window, 1) if step else mixed)
    results = []
    for part in range(plan.nx):
        result = moved[(-part) % plan.nx]
        for other in range(1, plan.nx):
            result = jnp.where(group == other, moved[(other - part) % plan.nx], result)
        results.append(result)
    return results


def middle_kernel(plan, in_ref, z_table_ref, y_forward_ref, y_inverse_ref, line_x_ref, line_y_ref, line_z_ref, out_ref, u_ref, o_ref, mid_ref):
    parity = lax.axis_index("gz")
    device = lax.axis_index("gy") * plan.nx + lax.axis_index("gx")
    row_k, pad_k = plan.row_k, plan.pad_k
    shape = (plan.pad_y, 2, pad_k, 2 * LANES)

    def z_transform(direction):
        high = z_table_ref[parity, direction, 0]
        both = jnp.concatenate([high, high], axis=0)
        total = mm(u_ref[...], both) + mm(u_ref[:, :LANES], z_table_ref[parity, direction, 1])
        return total.reshape(shape)

    def forward(gy, carry):
        def tile_step(tile, carry):
            here = pl.ds(pl.multiple_of(tile * LANES, LANES), LANES)
            values = [in_ref[gy * plan.nx + gx, :, here] for gx in range(plan.nx)]
            for part, value in enumerate(regroup(plan, values)):
                rows = pl.ds(pl.multiple_of((tile * plan.nx + part) * row_k, row_k), row_k)
                high, low = halves(value)
                u_ref[rows, :LANES] = high
                u_ref[rows, LANES:] = low
            return carry

        lax.fori_loop(0, plan.tiles, tile_step, 0)
        total = z_transform(0)
        real, imag = total[:, 0], total[:, 1]
        rows = pl.ds(pl.multiple_of(gy * (plan.pad_y * pad_k), pad_k), plan.pad_y * pad_k)
        mid_ref[0, rows, :] = (real[..., :LANES] + imag[..., LANES:]).reshape(-1, LANES)
        mid_ref[1, rows, :] = (imag[..., :LANES] - real[..., LANES:]).reshape(-1, LANES)
        return carry

    lax.fori_loop(0, plan.ny, forward, 0)

    def column(j, carry):
        lines = pl.ds(j, plan.all_y, stride=pad_k)
        real = mid_ref[0, lines, :]
        imag = mid_ref[1, lines, :]
        stacked = jnp.concatenate(
            [jnp.concatenate([real, imag], axis=1), jnp.concatenate([imag, -real], axis=1)], axis=0
        )
        high, low = halves(stacked)
        spectrum = mm(y_forward_ref[0], high) + (mm(y_forward_ref[0], low) + mm(y_forward_ref[1], high))
        kx = device * plan.width_k + j
        square = (line_y_ref[0] + line_z_ref[parity, 0]) + line_x_ref[0, kx]
        factor = (line_y_ref[1] * line_z_ref[parity, 1]) * line_x_ref[1, kx]
        green = jnp.where(
            square > 0.0,
            coulomb
            * jnp.exp(square * (-np.pi**2 / (ewald * ewald * GRID * GRID)))
            * factor
            / (np.pi * GRID * jnp.maximum(square, 1.0)),
            0.0,
        )
        real = spectrum[:, :LANES] * green
        imag = spectrum[:, LANES:] * green
        stacked = jnp.concatenate(
            [jnp.concatenate([real, imag], axis=1), jnp.concatenate([-imag, real], axis=1)], axis=0
        )
        high, low = halves(stacked)
        result = mm(y_inverse_ref[0], high) + (mm(y_inverse_ref[0], low) + mm(y_inverse_ref[1], high))
        mid_ref[0, lines, :] = result[:, :LANES]
        mid_ref[1, lines, :] = result[:, LANES:]
        return carry

    lax.fori_loop(0, plan.width_k, column, 0)

    def backward(gy, carry):
        rows = pl.ds(pl.multiple_of(gy * (plan.pad_y * pad_k), pad_k), plan.pad_y * pad_k)
        real = mid_ref[0, rows, :].reshape(plan.pad_y, pad_k, LANES)
        imag = mid_ref[1, rows, :].reshape(plan.pad_y, pad_k, LANES)
        high, low = halves(jnp.concatenate([real, imag], axis=1).reshape(-1, LANES))
        u_ref[:, :LANES] = high
        u_ref[:, LANES:] = low
        total = z_transform(1)
        real, imag = total[:, 0], total[:, 1]
        result = jnp.concatenate(
            [real[..., :LANES] - imag[..., LANES:], imag[..., :LANES] + real[..., LANES:]], axis=1
        )
        o_ref[...] = result.reshape(-1, LANES)

        def tile_step(tile, carry):
            values = []
            for part in range(plan.nx):
                rows = pl.ds(pl.multiple_of((tile * plan.nx + part) * row_k, row_k), row_k)
                values.append(o_ref[rows, :])
            here = pl.ds(pl.multiple_of(tile * LANES, LANES), LANES)
            for gx, value in enumerate(regroup(plan, values)):
                out_ref[gy * plan.nx + gx, :, here] = value
            return carry

        lax.fori_loop(0, plan.tiles, tile_step, 0)
        return carry

    lax.fori_loop(0, plan.ny, backward, 0)


def gather_kernel(plan, bounds_ref, atoms_ref, in_ref, dft_ref, out_ref, pot_ref, y_ref, z_ref, x_ref, p_ref, sum_ref):
    parity = lax.axis_index("gz")
    first = lax.axis_index("gx") * plan.window
    out_ref[...] = jnp.zeros_like(out_ref)
    x_ref[...] = jnp.zeros_like(x_ref)
    pack = plan.pack_x

    def transform(tile, carry):
        here = pl.ds(pl.multiple_of(tile * LANES, LANES), LANES)
        lines = in_ref[:, :, here].reshape(plan.dests * plan.row_k, LANES)
        high, low = halves(lines.T)
        first_pass = mm(jnp.concatenate([high, low], axis=0), dft_ref[0])
        value = first_pass[:LANES] + (first_pass[LANES:] + mm(high, dft_ref[1]))
        lane = lax.rem(lax.broadcasted_iota(jnp.int32, value.shape, 1), pack)
        rest = value - value.astype(jnp.bfloat16).astype(jnp.float32)
        value = jnp.where((lane >= plan.pad_x) & (lane < 2 * plan.pad_x), rest, value)
        for octet in range(plan.octets):
            for part in range(0, plan.nx, 2):
                pieces = []
                for other in range(2):
                    row = (part + other) * plan.window + octet * SUBLANES
                    pieces.append(value[row : row + SUBLANES])
                row = pl.multiple_of((tile * plan.nx + part) * SUBLANES, 2 * SUBLANES)
                pot_ref[octet, pl.ds(row, 2 * SUBLANES), :] = jnp.concatenate(pieces, axis=0).astype(jnp.bfloat16)
        return carry

    lax.fori_loop(0, plan.tiles, transform, 0)

    def work(block, chunk, meets):
        atoms = atoms_ref[block, :, pl.ds(pl.multiple_of(chunk * LANES, LANES), LANES)]
        weights, slopes = spline_rows(atoms[0:3])
        sign = fold_sign(parity, block // plan.nx)
        offset = offsets(plan.pad_x, atoms[4:5])
        table = jnp.concatenate([placed(offset, weights, 0), placed(offset, slopes, 0)], axis=1)
        high = table.astype(jnp.bfloat16).astype(jnp.float32)
        unused = jnp.zeros((pack - 3 * plan.pad_x, 2 * LANES), jnp.float32)
        x_ref[...] = jnp.concatenate([high, high, table - high, unused], axis=0).astype(jnp.bfloat16)
        offset = offsets(plan.pad_y, atoms[5:6])
        y_ref[0] = placed(offset, weights, 1)
        y_ref[1] = placed(offset, slopes, 1)
        z_ref[0] = z_rows(plan, weights, atoms[6:7], parity) * sign
        z_ref[1] = z_rows(plan, slopes, atoms[6:7], parity) * sign
        sum_ref[...] = jnp.zeros_like(sum_ref)
        place = pl.multiple_of(lax.rem(block, plan.nx) * pack, LANES)
        for octet in range(plan.octets):

            @pl.when(meets(first + octet * SUBLANES, SUBLANES))
            def _():
                p_ref[...] = mm(pot_ref[octet, :, pl.ds(place, pack)], x_ref[...])
                total_x = jnp.zeros((SUBLANES, LANES), jnp.float32)
                total_y = jnp.zeros((SUBLANES, LANES), jnp.float32)
                total_z = jnp.zeros((SUBLANES, LANES), jnp.float32)
                for y in range(plan.pad_y):
                    rows = slice(y * SUBLANES, (y + 1) * SUBLANES)
                    plain = p_ref[rows, :LANES]
                    weight = y_ref[0, y : y + 1]
                    total_x += weight * p_ref[rows, LANES:]
                    total_y += y_ref[1, y : y + 1] * plain
                    total_z += weight * plain
                lines = slice(octet * SUBLANES, (octet + 1) * SUBLANES)
                weight = z_ref[0, lines]
                sum_ref[0] += weight * total_x
                sum_ref[1] += weight * total_y
                sum_ref[2] += z_ref[1, lines] * total_z

        for dim in range(3):
            row = jnp.sum(sum_ref[dim], axis=0, keepdims=True)
            out_ref[block, pl.ds(dim * plan.chunks + chunk, 1), :] = row

    over_chunks(plan, bounds_ref, work)


def vmem_call(kernel, out_shape, scratch_shapes, smem=()):
    def call(*operands):
        specs = [
            pl.BlockSpec(memory_space=pltpu.SMEM if i in smem else pltpu.VMEM)
            for i in range(len(operands))
        ]
        return pl.pallas_call(
            kernel,
            in_specs=specs,
            out_specs=pl.BlockSpec(memory_space=pltpu.VMEM),
            out_shape=out_shape,
            scratch_shapes=scratch_shapes,
            compiler_params=pltpu.CompilerParams(vmem_limit_bytes=50 * 2**20),
        )(*operands)

    return call


def per_device(charges, fractions, base_cells, counts):
    capacity = charges.shape[0]
    plan = Plan(lax.axis_size("gz"), lax.axis_size("gy"), lax.axis_size("gx"), capacity)
    f32, bf16 = jnp.float32, jnp.bfloat16
    slot = jnp.arange(capacity, dtype=jnp.int32)
    live = slot < counts.reshape(())
    charge = jnp.where(live, charges, jnp.zeros_like(charges))
    local_x = (base_cells[0] - lax.axis_index("gx") * plan.cells_x).astype(f32)
    local_y = (base_cells[1] - lax.axis_index("gy") * plan.cells_y).astype(f32)
    key = jnp.where(live, base_cells[2] - lax.axis_index("gz") * plan.cells_z, plan.cells_z)
    key, slot, t_x, t_y, t_z, charge, local_x, local_y = lax.sort(
        [key, slot, fractions[0], fractions[1], fractions[2], charge, local_x, local_y],
        num_keys=1,
        is_stable=False,
    )
    atoms = jnp.stack([t_x, t_y, t_z, charge, local_x, local_y, key.astype(f32), jnp.zeros_like(t_x)])
    atoms = exchange(atoms, ("gz", "gx"), 0, same=True)
    low = atoms[:, 6, ::LANES]
    high = jnp.minimum(atoms[:, 6, LANES - 1 :: LANES], plan.cells_z - 1.0)
    high = jnp.where(low < plan.cells_z, high, -2.0 * plan.halo)
    bounds = jnp.stack([low, high]).astype(jnp.int32).reshape(2, -1)

    lanes = plan.tiles * LANES
    half_shape = jax.ShapeDtypeStruct((plan.dests, plan.row_k, lanes), f32)
    data = vmem_call(
        functools.partial(spread_kernel, plan),
        half_shape,
        [
            pltpu.VMEM((plan.octets, plan.rows, plan.nx * LANES), f32),
            pltpu.VMEM((plan.pad_y, LANES), f32),
            pltpu.VMEM((plan.window, LANES), f32),
            pltpu.VMEM((2 * LANES, 2 * LANES), bf16),
            pltpu.VMEM((plan.rows, 2 * LANES), bf16),
        ],
        smem=(0,),
    )(bounds, atoms, plan.x_forward())
    data = exchange(data, ("gy", "gx"), 1)
    y_forward, y_inverse = plan.y_tables()
    line_x, line_y, line_z = plan.green_lines()
    data = vmem_call(
        functools.partial(middle_kernel, plan),
        half_shape,
        [
            pltpu.VMEM((plan.pad_y * plan.row_k, 2 * LANES), bf16),
            pltpu.VMEM((plan.pad_y * plan.row_k, LANES), f32),
            pltpu.VMEM((2, plan.all_y * plan.pad_k, LANES), f32),
        ],
        smem=(4,),
    )(data, plan.z_tables(), y_forward, y_inverse, line_x, line_y, line_z)
    data = exchange(data, ("gy", "gx"), 2)
    parts = vmem_call(
        functools.partial(gather_kernel, plan),
        jax.ShapeDtypeStruct((plan.blocks, 3 * plan.chunks, LANES), f32),
        [
            pltpu.VMEM((plan.octets, plan.rows, plan.nx * plan.pack_x), bf16),
            pltpu.VMEM((2, plan.pad_y, LANES), f32),
            pltpu.VMEM((2, plan.window, LANES), f32),
            pltpu.VMEM((plan.pack_x, 2 * LANES), bf16),
            pltpu.VMEM((plan.rows, 2 * LANES), f32),
            pltpu.VMEM((3, SUBLANES, LANES), f32),
        ],
        smem=(0,),
    )(bounds, atoms, data, plan.x_inverse())
    parts = exchange(parts, ("gz", "gx"), 3)
    forces = -charge[None, :] * jnp.sum(parts, axis=0).reshape(3, capacity)
    result = lax.sort([slot, forces[0], forces[1], forces[2]], num_keys=1, is_stable=False)
    return jnp.stack(result[1:])


def solution(mesh):
    in_specs = (
        P(("gz", "gy", "gx")),
        P(None, ("gz", "gy", "gx")),
        P(None, ("gz", "gy", "gx")),
        P("gz", "gy", "gx"),
    )
    out_specs = P(None, ("gz", "gy", "gx"))
    return jax.shard_map(
        per_device, mesh=mesh, in_specs=in_specs, out_specs=out_specs, check_vma=False
    )
```

```python
import functools

import jax
import jax.numpy as jnp
import numpy as np
from jax import lax
from jax.experimental import pallas as pl
from jax.experimental.pallas import tpu as pltpu
from jax.sharding import PartitionSpec as P

GRID = 256
ORDER = 4
LANES = 128
SUBLANES = 8

coulomb = 332.0636
ewald = 0.7
MESH = pl.DeviceIdType.MESH
ROWS_BY_ROWS = (((1,), (1,)), ((), ()))


def round_up(value, unit):
    return -(-value // unit) * unit


def halves(value):
    high = value.astype(jnp.bfloat16)
    low = (value - high.astype(jnp.float32)).astype(jnp.bfloat16)
    return high, low


def constant_halves(value):
    value = np.asarray(value, np.float32)
    high = value.astype(jnp.bfloat16)
    low = (value - high.astype(np.float32)).astype(jnp.bfloat16)
    return jnp.asarray(np.stack([high, low]))


def mm(a, b, contract=(((1,), (0,)), ((), ()))):
    return lax.dot_general(a, b, contract, preferred_element_type=jnp.float32)


class Plan:
    def __init__(self, nz, ny, nx, capacity):
        self.nz, self.ny, self.nx = nz, ny, nx
        self.capacity = capacity
        self.chunks = capacity // LANES
        self.blocks = nz * nx
        self.cells_x = GRID // nx
        self.cells_y = GRID // ny
        self.cells_z = GRID // nz
        self.halo = ORDER - 1
        self.span_x = self.cells_x + self.halo
        self.span_y = self.cells_y + self.halo
        self.window = self.cells_z // nx
        self.octets = self.window // SUBLANES
        self.tiles = -(-self.span_y // nx)
        self.pad_y = self.tiles * nx
        self.rows = self.pad_y * SUBLANES
        self.dests = ny * nx
        self.kept = GRID // 2
        self.width_k = self.kept // self.dests
        self.pad_k = round_up(self.width_k, SUBLANES)
        self.row_k = 2 * self.pad_k
        self.all_y = ny * self.pad_y
        self.pad_x = round_up(self.span_x, SUBLANES)
        self.pack_x = round_up(3 * self.pad_x, LANES)
        self.unroll = 4
        sizes = [len(part) for part in np.array_split(np.arange(self.tiles), 4)]
        self.parts = [(sum(sizes[:i]), size) for i, size in enumerate(sizes)]
        self.most = max(sizes)
        assert nz == 2 and self.cells_z == LANES and self.span_x <= LANES

    def angle(self, outputs, inputs):
        return (outputs[:, None] * inputs[None, :] % GRID) * (2.0 * np.pi / GRID)

    def index_kx(self):
        place = np.arange(self.pad_k)
        index = np.arange(self.dests)[:, None] * self.width_k + np.minimum(place, self.width_k - 1)[None, :]
        return index.reshape(-1), np.tile(place < self.width_k, self.dests)

    def pairs(self, cosine, sine):
        shape = (self.dests, 1, self.pad_k, -1)
        both = np.concatenate([cosine.reshape(shape), sine.reshape(shape)], axis=1)
        return both.reshape(self.dests * self.row_k, -1)

    def x_forward(self):
        local = np.arange(LANES)
        cells = (np.arange(self.nx)[:, None] * self.cells_x + local[None, :]).reshape(-1)
        used = np.tile(local < self.span_x, self.nx)
        index, kept = self.index_kx()
        angle = self.angle(index, cells)
        mask = kept[:, None] * used[None, :]
        return constant_halves(self.pairs(np.cos(angle) * mask, -np.sin(angle) * mask))

    def x_inverse(self):
        lane = np.arange(self.pack_x)
        local = lane % self.pad_x
        cells = (np.arange(self.nx)[:, None] * self.cells_x + local[None, :]).reshape(-1)
        used = np.tile((local < self.span_x) & (lane < 3 * self.pad_x), self.nx)
        index, kept = self.index_kx()
        angle = self.angle(index, cells)
        mask = (kept * np.where(index > 0, 2.0, 1.0))[:, None] * used[None, :]
        return constant_halves(self.pairs(np.cos(angle) * mask, -np.sin(angle) * mask))

    def z_tables(self):
        cells = np.arange(self.cells_z)
        tables = []
        for parity in range(self.nz):
            angle = self.angle(self.nz * cells + parity, cells)
            forward = np.concatenate([np.cos(angle).T, np.sin(angle).T], axis=1)
            inverse = np.concatenate([np.cos(angle), np.sin(angle)], axis=1)
            tables += [constant_halves(forward), constant_halves(inverse)]
        return jnp.stack(tables).reshape(self.nz, 2, 2, self.cells_z, 2 * self.cells_z)

    def y_tables(self):
        local = np.arange(self.pad_y)
        cells = (np.arange(self.ny)[:, None] * self.cells_y + local[None, :]).reshape(-1)
        used = np.tile(local < self.span_y, self.ny)
        angle = self.angle(np.arange(GRID), cells)
        cosine, sine = np.cos(angle) * used[None, :], np.sin(angle) * used[None, :]
        forward = constant_halves(np.concatenate([cosine, sine], axis=1))
        inverse = constant_halves(np.concatenate([cosine.T, sine.T], axis=1))
        return forward, inverse

    def green_lines(self):
        index = np.arange(GRID)
        signed = np.where(2 * index < GRID, index, index - GRID)
        square = (signed * signed).astype(np.float32)
        bspline = 36.0 / (4.0 + 2.0 * np.cos(index * (2.0 * np.pi / GRID))) ** 2
        bspline = np.where(2 * index == GRID, 0.0, bspline).astype(np.float32)
        line_x = np.stack([square, bspline])[:, : self.kept]
        line_y = np.stack([square, bspline])[:, :, None]
        line_z = np.stack([square, bspline]).reshape(2, 1, self.cells_z, self.nz)
        line_z = line_z.transpose(3, 0, 1, 2)
        return jnp.asarray(line_x), jnp.asarray(line_y), jnp.asarray(line_z)


def flipped(value, size, mask):
    result, bit = 0, 1
    while bit < size:
        digit = value // bit % 2
        result = result + bit * ((digit + mask // bit % 2) % 2)
        bit *= 2
    return result


class Group:
    def __init__(self, axes, sizes):
        self.axes, self.sizes = axes, sizes
        self.count = int(np.prod(sizes))
        self.steps = sorted(range(1, self.count), key=lambda mask: -bin(mask).count("1"))

    def index(self, coordinates):
        place = 0
        for axis, size in zip(self.axes, self.sizes):
            place = place * size + coordinates[axis]
        return place

    def me(self):
        return self.index({axis: lax.axis_index(axis) for axis in self.axes})

    def partner(self, mask):
        where = {}
        for axis, size in reversed(list(zip(self.axes, self.sizes))):
            where[axis] = flipped(lax.axis_index(axis), size, mask % size)
            mask //= size
        return where

    def barrier(self):
        semaphore = pltpu.get_barrier_semaphore()
        for step in self.steps:
            pl.semaphore_signal(
                semaphore, inc=1, device_id=self.partner(step), device_id_type=MESH
            )
        pl.semaphore_wait(semaphore, self.count - 1)

    def copies(self, source, target, send_sems, recv_sems):
        result = []
        for step in self.steps:
            where = self.partner(step)
            result.append(
                pltpu.make_async_remote_copy(
                    src_ref=source(self.index(where)),
                    dst_ref=target(self.me()),
                    send_sem=send_sems(step),
                    recv_sem=recv_sems(step),
                    device_id=where,
                    device_id_type=MESH,
                )
            )
        return result


def exchange_kernel(group, same, src_ref, out_ref, send_sems, recv_sems, local_sem):
    me = group.me()
    group.barrier()
    copies = group.copies(
        lambda peer: src_ref if same else src_ref.at[peer],
        lambda place: out_ref.at[place],
        lambda step: send_sems.at[step],
        lambda step: recv_sems.at[step],
    )
    for copy in copies:
        copy.start()
    own = pltpu.make_async_copy(src_ref if same else src_ref.at[me], out_ref.at[me], local_sem)
    own.start()
    own.wait()
    for copy in copies:
        copy.wait()


def group_of(*axes):
    return Group(axes, [lax.axis_size(axis) for axis in axes])


def exchange(data, group, collective_id, same=False):
    shape = ((group.count,) if same else ()) + data.shape
    return pl.pallas_call(
        functools.partial(exchange_kernel, group, same),
        in_specs=[pl.BlockSpec(memory_space=pltpu.VMEM)],
        out_specs=pl.BlockSpec(memory_space=pltpu.VMEM),
        out_shape=jax.ShapeDtypeStruct(shape, data.dtype),
        scratch_shapes=[
            pltpu.SemaphoreType.DMA((group.count,)),
            pltpu.SemaphoreType.DMA((group.count,)),
            pltpu.SemaphoreType.DMA,
        ],
        compiler_params=pltpu.CompilerParams(
            collective_id=collective_id, has_side_effects=True
        ),
    )(data)


def spline_rows(frac):
    rest = 1.0 - frac
    square = frac * frac
    cube = square * frac
    weights = [
        rest * rest * rest / 6.0,
        (3.0 * cube - 6.0 * square + 4.0) / 6.0,
        (-3.0 * cube + 3.0 * square + 3.0 * frac + 1.0) / 6.0,
        cube / 6.0,
    ]
    slopes = [
        -0.5 * rest * rest,
        1.5 * square - 2.0 * frac,
        -1.5 * square + frac + 0.5,
        0.5 * square,
    ]
    return weights, slopes


def placed(offset, values, dim):
    total = jnp.zeros(offset.shape, jnp.float32)
    for k in range(ORDER):
        total = jnp.where(offset == float(k), values[k][dim : dim + 1], total)
    return total


def offsets(rows, lowest):
    return lax.broadcasted_iota(jnp.int32, (rows, LANES), 0).astype(jnp.float32) - lowest


def fold_sign(parity, part):
    return (1 - 2 * lax.rem(parity * part, 2)).astype(jnp.float32)


def list_units(plan, counts_ref, list_ref):
    place = lax.axis_index("gx")

    def block_step(block, total):
        def listed(octet, begin, end, total):
            def put(chunk, total):
                list_ref[total] = (block * plan.chunks + chunk) * plan.octets + octet
                return total + 1

            return lax.fori_loop(begin, end, put, total)

        ends = 0
        for octet in range(plan.octets):
            start = counts_ref[block, place * plan.octets + octet]
            stop = counts_ref[block, LANES // 2 + place * plan.octets + octet]
            begin = start // LANES
            end = jnp.where(stop > start, (stop + LANES - 1) // LANES, begin)
            if octet == 0:
                ends = jnp.where(stop > start, end, 0)
            total = listed(octet, begin, end, total)
        start = counts_ref[block, plan.nx * plan.octets]
        stop = counts_ref[block, LANES // 2 + plan.nx * plan.octets]
        begin = jnp.maximum(start // LANES, ends)
        end = jnp.where((stop > start) & (place == 0), (stop + LANES - 1) // LANES, begin)
        return listed(0, begin, end, total)

    total = lax.fori_loop(0, plan.blocks, block_step, 0)
    for extra in range(plan.unroll):
        list_ref[total + extra] = 0
    return total


def over_units(plan, counts_ref, list_ref, work):
    total = list_units(plan, counts_ref, list_ref)
    parity = lax.axis_index("gz")

    def step(i, carry):
        for lane in range(plan.unroll):
            unit = i * plan.unroll + lane
            code = list_ref[unit]
            octet = lax.rem(code, plan.octets)
            code = lax.div(code, plan.octets)
            chunk, block = lax.rem(code, plan.chunks), lax.div(code, plan.chunks)
            sign = fold_sign(parity, block // plan.nx)
            work(lane, block, chunk, octet, jnp.where(unit < total, sign, 0.0))
        return carry

    lax.fori_loop(0, (total + plan.unroll - 1) // plan.unroll, step, 0)


def z_offsets(plan, octet, lowest):
    first = lax.axis_index("gx") * plan.window + octet * SUBLANES
    offset = offsets(SUBLANES, lowest - first.astype(jnp.float32))
    wraps = offset < float(ORDER - plan.cells_z)
    factor = jnp.where(wraps, fold_sign(lax.axis_index("gz"), 1), 1.0)
    return jnp.where(wraps, offset + float(plan.cells_z), offset), factor


def spread_kernel(plan, counts_ref, atoms_ref, grid_ref, list_ref, y_ref, x_ref, a_ref):
    grid_ref[...] = jnp.zeros_like(grid_ref)
    x_ref[...] = jnp.zeros_like(x_ref)

    def work(lane, block, chunk, octet, sign):
        atoms = atoms_ref[block, :, pl.ds(pl.multiple_of(chunk * LANES, LANES), LANES)]
        weights, _ = spline_rows(atoms[0:3])
        high, low = halves(
            jnp.concatenate(
                [
                    placed(offsets(plan.pad_x, atoms[4:5]), weights, 0),
                    jnp.zeros((LANES - plan.pad_x, LANES), jnp.float32),
                ],
                axis=0,
            )
        )
        x_ref[lane, :LANES, :LANES] = high
        x_ref[lane, :LANES, LANES:] = high
        x_ref[lane, LANES:, :LANES] = low
        y_ref[lane] = placed(offsets(plan.pad_y, atoms[5:6]), weights, 1)
        offset, factor = z_offsets(plan, octet, atoms[6:7])
        line = placed(offset, weights, 2) * factor * (atoms[3:4] * sign)
        for y in range(0, plan.pad_y, 2):
            pair = jnp.concatenate([y_ref[lane, y : y + 1] * line, y_ref[lane, y + 1 : y + 2] * line], axis=0)
            high, low = halves(pair)
            a_ref[lane, y * SUBLANES : (y + 2) * SUBLANES, :LANES] = high
            a_ref[lane, y * SUBLANES : (y + 2) * SUBLANES, LANES:] = low
        product = mm(a_ref[lane], x_ref[lane], ROWS_BY_ROWS)
        place = pl.ds(pl.multiple_of(lax.rem(block, plan.nx) * LANES, LANES), LANES)
        grid_ref[octet, :, place] += product[:, :LANES] + product[:, LANES:]

    over_units(plan, counts_ref, list_ref, work)


def regroup(plan, values):
    shape = values[0].shape
    group = lax.broadcasted_iota(jnp.int32, shape, 1) // plan.window
    moved = []
    for step in range(plan.nx):
        mixed = values[step % plan.nx]
        for part in range(1, plan.nx):
            mixed = jnp.where(group == part, values[(part + step) % plan.nx], mixed)
        moved.append(pltpu.roll(mixed, step * plan.window, 1) if step else mixed)
    results = []
    for part in range(plan.nx):
        result = moved[(-part) % plan.nx]
        for other in range(1, plan.nx):
            result = jnp.where(group == other, moved[(other - part) % plan.nx], result)
        results.append(result)
    return results


def mesh_kernel(
    plan,
    group,
    grid_ref,
    x_forward_ref,
    z_table_ref,
    y_forward_ref,
    y_inverse_ref,
    line_x_ref,
    line_y_ref,
    line_z_ref,
    x_inverse_ref,
    pot_ref,
    there_out_ref,
    there_in_ref,
    back_out_ref,
    back_in_ref,
    u_ref,
    o_ref,
    mid_ref,
    send_sems,
    recv_sems,
    local_sems,
):
    parity = lax.axis_index("gz")
    device = group.me()
    row_k, pad_k, nx = plan.row_k, plan.pad_k, plan.nx
    group.barrier()

    def sending(way, part, out_ref, in_ref):
        first, count = plan.parts[part]
        lanes = pl.ds(first * LANES, count * LANES)
        copies = group.copies(
            lambda peer: out_ref.at[peer, :, lanes],
            lambda place: in_ref.at[place, :, lanes],
            lambda step: send_sems.at[way, part, step],
            lambda step: recv_sems.at[way, part, step],
        )
        own = pltpu.make_async_copy(
            out_ref.at[device, :, lanes], in_ref.at[device, :, lanes], local_sems.at[way, part]
        )
        return copies, own

    def start(copies, own):
        for copy in copies:
            copy.start()
        own.start()

    def arrive(copies, own):
        for copy in copies:
            copy.wait_recv()
        own.wait()

    def tile_lanes(tile):
        return pl.ds(pl.multiple_of(tile * LANES, LANES), LANES)

    def x_forward(tile, carry):
        pieces = []
        for other in range(nx):
            row = pl.multiple_of((tile * nx + other) * SUBLANES, SUBLANES)
            for octet in range(plan.octets):
                pieces.append(grid_ref[octet, pl.ds(row, SUBLANES), :])
        high, low = halves(jnp.concatenate(pieces, axis=0))
        first_pass = mm(x_forward_ref[0], jnp.concatenate([high, low], axis=0), ROWS_BY_ROWS)
        second_pass = mm(x_forward_ref[1], high, ROWS_BY_ROWS)
        total = first_pass[:, :LANES] + (first_pass[:, LANES:] + second_pass)
        there_out_ref[:, :, tile_lanes(tile)] = total.reshape(plan.dests, row_k, LANES)
        return carry

    there = [sending(0, part, there_out_ref, there_in_ref) for part in range(len(plan.parts))]
    back = [sending(1, part, back_out_ref, back_in_ref) for part in range(len(plan.parts))]
    for part, (first, count) in enumerate(plan.parts):
        lax.fori_loop(first, first + count, x_forward, 0)
        start(*there[part])

    def z_transform(direction, rows):
        high = z_table_ref[parity, direction, 0]
        both = jnp.concatenate([high, high], axis=0)
        low = z_table_ref[parity, direction, 1]
        total = mm(u_ref[:rows], both) + mm(u_ref[:rows, :LANES], low)
        return total.reshape(rows // row_k, 2, pad_k, 2 * LANES)

    for part, (first, count) in enumerate(plan.parts):
        arrive(*there[part])
        lines = count * nx

        def z_forward(gy, carry):
            for tile in range(count):
                here = pl.ds((first + tile) * LANES, LANES)
                values = [there_in_ref[gy * nx + gx, :, here] for gx in range(nx)]
                for other, value in enumerate(regroup(plan, values)):
                    row = (tile * nx + other) * row_k
                    high, low = halves(value)
                    u_ref[row : row + row_k, :LANES] = high
                    u_ref[row : row + row_k, LANES:] = low
            total = z_transform(0, lines * row_k)
            real, imag = total[:, 0], total[:, 1]
            row = pl.multiple_of((gy * plan.pad_y + first * nx) * pad_k, pad_k)
            rows = pl.ds(row, lines * pad_k)
            mid_ref[0, rows, :] = (real[..., :LANES] + imag[..., LANES:]).reshape(-1, LANES)
            mid_ref[1, rows, :] = (imag[..., :LANES] - real[..., LANES:]).reshape(-1, LANES)
            return carry

        lax.fori_loop(0, plan.ny, z_forward, 0)

    def column(j):
        lines = pl.ds(j, plan.all_y, stride=pad_k)
        real = mid_ref[0, lines, :]
        imag = mid_ref[1, lines, :]
        stacked = jnp.concatenate(
            [jnp.concatenate([real, imag], axis=1), jnp.concatenate([imag, -real], axis=1)], axis=0
        )
        high, low = halves(stacked)
        spectrum = mm(y_forward_ref[0], high) + (mm(y_forward_ref[0], low) + mm(y_forward_ref[1], high))
        kx = device * plan.width_k + j
        square = (line_y_ref[0] + line_z_ref[parity, 0]) + line_x_ref[0, kx]
        factor = (line_y_ref[1] * line_z_ref[parity, 1]) * line_x_ref[1, kx]
        green = jnp.where(
            square > 0.0,
            coulomb
            * jnp.exp(square * (-np.pi**2 / (ewald * ewald * GRID * GRID)))
            * factor
            / (np.pi * GRID * jnp.maximum(square, 1.0)),
            0.0,
        )
        real = spectrum[:, :LANES] * green
        imag = spectrum[:, LANES:] * green
        stacked = jnp.concatenate(
            [jnp.concatenate([real, imag], axis=1), jnp.concatenate([-imag, real], axis=1)], axis=0
        )
        high, low = halves(stacked)
        result = mm(y_inverse_ref[0], high) + (mm(y_inverse_ref[0], low) + mm(y_inverse_ref[1], high))
        return lines, result

    def columns(i, carry):
        results = [column(i * 2 + other) for other in range(2)]
        for lines, result in results:
            mid_ref[0, lines, :] = result[:, :LANES]
            mid_ref[1, lines, :] = result[:, LANES:]
        return carry

    lax.fori_loop(0, plan.width_k // 2, columns, 0)

    for part, (first, count) in enumerate(plan.parts):
        lines = count * nx

        def z_backward(gy, carry):
            row = pl.multiple_of((gy * plan.pad_y + first * nx) * pad_k, pad_k)
            rows = pl.ds(row, lines * pad_k)
            real = mid_ref[0, rows, :].reshape(lines, pad_k, LANES)
            imag = mid_ref[1, rows, :].reshape(lines, pad_k, LANES)
            high, low = halves(jnp.concatenate([real, imag], axis=1).reshape(-1, LANES))
            u_ref[: lines * row_k, :LANES] = high
            u_ref[: lines * row_k, LANES:] = low
            total = z_transform(1, lines * row_k)
            real, imag = total[:, 0], total[:, 1]
            result = jnp.concatenate(
                [real[..., :LANES] - imag[..., LANES:], imag[..., :LANES] + real[..., LANES:]], axis=1
            )
            o_ref[: lines * row_k] = result.reshape(-1, LANES)
            for tile in range(count):
                values = []
                for other in range(nx):
                    row = (tile * nx + other) * row_k
                    values.append(o_ref[row : row + row_k])
                here = pl.ds((first + tile) * LANES, LANES)
                for gx, value in enumerate(regroup(plan, values)):
                    back_out_ref[gy * nx + gx, :, here] = value
            return carry

        lax.fori_loop(0, plan.ny, z_backward, 0)
        start(*back[part])

    def x_inverse(tile, carry):
        lines = back_in_ref[:, :, tile_lanes(tile)].reshape(plan.dests * row_k, LANES)
        high, low = halves(lines.T)
        first_pass = mm(jnp.concatenate([high, low], axis=0), x_inverse_ref[0])
        value = first_pass[:LANES] + (first_pass[LANES:] + mm(high, x_inverse_ref[1]))
        lane = lax.rem(lax.broadcasted_iota(jnp.int32, value.shape, 1), plan.pack_x)
        rest = value - value.astype(jnp.bfloat16).astype(jnp.float32)
        value = jnp.where((lane >= plan.pad_x) & (lane < 2 * plan.pad_x), rest, value)
        for octet in range(plan.octets):
            for other in range(0, nx, 2):
                pieces = []
                for extra in range(2):
                    row = (other + extra) * plan.window + octet * SUBLANES
                    pieces.append(value[row : row + SUBLANES])
                row = pl.multiple_of((tile * nx + other) * SUBLANES, 2 * SUBLANES)
                pot_ref[octet, pl.ds(row, 2 * SUBLANES), :] = jnp.concatenate(pieces, axis=0).astype(jnp.bfloat16)
        return carry

    for part, (first, count) in enumerate(plan.parts):
        arrive(*back[part])
        lax.fori_loop(first, first + count, x_inverse, 0)
    for copies, _ in there + back:
        for copy in copies:
            copy.wait_send()


def gather_kernel(plan, counts_ref, atoms_ref, pot_ref, out_ref, list_ref, y_ref, x_ref, p_ref):
    out_ref[...] = jnp.zeros_like(out_ref)
    pack = plan.pack_x

    def work(lane, block, chunk, octet, sign):
        atoms = atoms_ref[block, :, pl.ds(pl.multiple_of(chunk * LANES, LANES), LANES)]
        weights, slopes = spline_rows(atoms[0:3])
        offset = offsets(plan.pad_x, atoms[4:5])
        table = jnp.concatenate([placed(offset, weights, 0), placed(offset, slopes, 0)], axis=1)
        high = table.astype(jnp.bfloat16).astype(jnp.float32)
        unused = jnp.zeros((pack - 3 * plan.pad_x, 2 * LANES), jnp.float32)
        x_ref[lane] = jnp.concatenate([high, high, table - high, unused], axis=0).astype(jnp.bfloat16)
        offset = offsets(plan.pad_y, atoms[5:6])
        y_ref[lane, 0] = placed(offset, weights, 1)
        y_ref[lane, 1] = placed(offset, slopes, 1)
        offset, factor = z_offsets(plan, octet, atoms[6:7])
        factor = factor * sign
        weight_z = placed(offset, weights, 2) * factor
        slope_z = placed(offset, slopes, 2) * factor
        place = pl.ds(pl.multiple_of(lax.rem(block, plan.nx) * pack, LANES), pack)
        p_ref[lane] = mm(pot_ref[octet, :, place], x_ref[lane])
        total_x = jnp.zeros((SUBLANES, LANES), jnp.float32)
        total_y = jnp.zeros((SUBLANES, LANES), jnp.float32)
        total_z = jnp.zeros((SUBLANES, LANES), jnp.float32)
        for y in range(plan.pad_y):
            rows = slice(y * SUBLANES, (y + 1) * SUBLANES)
            plain = p_ref[lane, rows, :LANES]
            weight = y_ref[lane, 0, y : y + 1]
            total_x += weight * p_ref[lane, rows, LANES:]
            total_y += y_ref[lane, 1, y : y + 1] * plain
            total_z += weight * plain
        totals = [weight_z * total_x, weight_z * total_y, slope_z * total_z]
        for dim in range(3):
            row = jnp.sum(totals[dim], axis=0, keepdims=True)
            out_ref[block, pl.ds(dim * plan.chunks + chunk, 1), :] += row

    over_units(plan, counts_ref, list_ref, work)


def vmem_call(kernel, out_shape, scratch_shapes, smem=(), **params):
    def call(*operands):
        specs = [
            pl.BlockSpec(memory_space=pltpu.SMEM if i in smem else pltpu.VMEM)
            for i in range(len(operands))
        ]
        return pl.pallas_call(
            kernel,
            in_specs=specs,
            out_specs=pl.BlockSpec(memory_space=pltpu.VMEM),
            out_shape=out_shape,
            scratch_shapes=scratch_shapes,
            compiler_params=pltpu.CompilerParams(vmem_limit_bytes=50 * 2**20, **params),
        )(*operands)

    return call


def per_device(charges, fractions, base_cells, counts):
    capacity = charges.shape[0]
    plan = Plan(lax.axis_size("gz"), lax.axis_size("gy"), lax.axis_size("gx"), capacity)
    f32, bf16 = jnp.float32, jnp.bfloat16
    slot = jnp.arange(capacity, dtype=jnp.int32)
    live = slot < counts.reshape(())
    charge = jnp.where(live, charges, jnp.zeros_like(charges))
    local_x = (base_cells[0] - lax.axis_index("gx") * plan.cells_x).astype(f32)
    local_y = (base_cells[1] - lax.axis_index("gy") * plan.cells_y).astype(f32)
    key = jnp.where(live, base_cells[2] - lax.axis_index("gz") * plan.cells_z, plan.cells_z)
    key, slot, t_x, t_y, t_z, charge, local_x, local_y = lax.sort(
        [key, slot, fractions[0], fractions[1], fractions[2], charge, local_x, local_y],
        num_keys=1,
        is_stable=False,
    )
    edges = np.full(LANES, -1)
    starts = np.arange(plan.nx * plan.octets + 1) * SUBLANES
    edges[: len(starts)] = starts - plan.halo
    edges[LANES // 2 : LANES // 2 + len(starts)] = np.minimum(starts + SUBLANES, plan.cells_z)
    counted = jnp.sum((key[None, :] < jnp.asarray(edges)[:, None]).astype(f32), axis=1)
    counted = jnp.pad(counted, (0, capacity - LANES))
    atoms = jnp.stack([t_x, t_y, t_z, charge, local_x, local_y, key.astype(f32), counted])
    atoms = exchange(atoms, group_of("gz", "gx"), 0, same=True)
    counts = atoms[:, 7, :LANES].astype(jnp.int32)

    lanes = plan.tiles * LANES
    mesh_shape = (plan.octets, plan.rows, plan.nx * LANES)
    units = plan.blocks * plan.chunks * plan.octets + plan.unroll
    grid = vmem_call(
        functools.partial(spread_kernel, plan),
        jax.ShapeDtypeStruct(mesh_shape, f32),
        [
            pltpu.SMEM((units,), jnp.int32),
            pltpu.VMEM((plan.unroll, plan.pad_y, LANES), f32),
            pltpu.VMEM((plan.unroll, 2 * LANES, 2 * LANES), bf16),
            pltpu.VMEM((plan.unroll, plan.rows, 2 * LANES), bf16),
        ],
        smem=(0,),
    )(counts, atoms)
    y_forward, y_inverse = plan.y_tables()
    line_x, line_y, line_z = plan.green_lines()
    group = group_of("gy", "gx")
    parts = len(plan.parts)
    half = pltpu.VMEM((plan.dests, plan.row_k, lanes), f32)
    potential = vmem_call(
        functools.partial(mesh_kernel, plan, group),
        jax.ShapeDtypeStruct((plan.octets, plan.rows, plan.nx * plan.pack_x), bf16),
        [
            half,
            half,
            half,
            half,
            pltpu.VMEM((plan.most * plan.nx * plan.row_k, 2 * LANES), bf16),
            pltpu.VMEM((plan.most * plan.nx * plan.row_k, LANES), f32),
            pltpu.VMEM((2, plan.all_y * plan.pad_k, LANES), f32),
            pltpu.SemaphoreType.DMA((2, parts, group.count)),
            pltpu.SemaphoreType.DMA((2, parts, group.count)),
            pltpu.SemaphoreType.DMA((2, parts)),
        ],
        smem=(5,),
        collective_id=1,
        has_side_effects=True,
    )(
        grid,
        plan.x_forward(),
        plan.z_tables(),
        y_forward,
        y_inverse,
        line_x,
        line_y,
        line_z,
        plan.x_inverse(),
    )
    shares = vmem_call(
        functools.partial(gather_kernel, plan),
        jax.ShapeDtypeStruct((plan.blocks, 3 * plan.chunks, LANES), f32),
        [
            pltpu.SMEM((units,), jnp.int32),
            pltpu.VMEM((plan.unroll, 2, plan.pad_y, LANES), f32),
            pltpu.VMEM((plan.unroll, plan.pack_x, 2 * LANES), bf16),
            pltpu.VMEM((plan.unroll, plan.rows, 2 * LANES), f32),
        ],
        smem=(0,),
    )(counts, atoms, potential)
    shares = exchange(shares, group_of("gz", "gx"), 2)
    forces = -charge[None, :] * jnp.sum(shares, axis=0).reshape(3, capacity)
    result = lax.sort([slot, forces[0], forces[1], forces[2]], num_keys=1, is_stable=False)
    return jnp.stack(result[1:])


def solution(mesh):
    in_specs = (
        P(("gz", "gy", "gx")),
        P(None, ("gz", "gy", "gx")),
        P(None, ("gz", "gy", "gx")),
        P("gz", "gy", "gx"),
    )
    out_specs = P(None, ("gz", "gy", "gx"))
    return jax.shard_map(
        per_device, mesh=mesh, in_specs=in_specs, out_specs=out_specs, check_vma=False
    )
```

```python
import functools

import jax
import jax.numpy as jnp
import numpy as np
from jax import lax
from jax.experimental import pallas as pl
from jax.experimental.pallas import tpu as pltpu
from jax.sharding import PartitionSpec as P

GRID = 256
ORDER = 4
LANES = 128
SUBLANES = 8

coulomb = 332.0636
ewald = 0.7
MESH = pl.DeviceIdType.MESH
ROWS_BY_ROWS = (((1,), (1,)), ((), ()))


def round_up(value, unit):
    return -(-value // unit) * unit


def halves(value):
    high = value.astype(jnp.bfloat16)
    low = (value - high.astype(jnp.float32)).astype(jnp.bfloat16)
    return high, low


def constant_halves(value):
    value = np.asarray(value, np.float32)
    high = value.astype(jnp.bfloat16)
    low = (value - high.astype(np.float32)).astype(jnp.bfloat16)
    return jnp.asarray(np.stack([high, low]))


def mm(a, b, contract=(((1,), (0,)), ((), ()))):
    return lax.dot_general(a, b, contract, preferred_element_type=jnp.float32)


class Plan:
    def __init__(self, nz, ny, nx, capacity):
        self.nz, self.ny, self.nx = nz, ny, nx
        self.capacity = capacity
        self.chunks = capacity // LANES
        self.blocks = nz * nx
        self.cells_x = GRID // nx
        self.cells_y = GRID // ny
        self.cells_z = GRID // nz
        self.halo = ORDER - 1
        self.span_x = self.cells_x + self.halo
        self.span_y = self.cells_y + self.halo
        self.window = self.cells_z // nx
        self.octets = self.window // SUBLANES
        self.tiles = -(-self.span_y // nx)
        self.pad_y = self.tiles * nx
        self.rows = self.pad_y * SUBLANES
        self.dests = ny * nx
        self.kept = GRID // 2
        self.width_k = self.kept // self.dests
        self.half_k = SUBLANES // 2
        self.groups = -(-self.width_k // self.half_k)
        self.row_k = self.groups * SUBLANES
        self.all_y = ny * self.pad_y
        self.pad_x = round_up(self.span_x, SUBLANES)
        self.pack_x = round_up(3 * self.pad_x, LANES)
        self.unroll = 4
        sizes = [len(part) for part in np.array_split(np.arange(self.tiles), 4)]
        self.parts = [(sum(sizes[:i]), size) for i, size in enumerate(sizes)]
        assert nz == 2 and self.cells_z == LANES and self.span_x <= LANES

    def angle(self, outputs, inputs):
        return (outputs[:, None] * inputs[None, :] % GRID) * (2.0 * np.pi / GRID)

    def index_kx(self):
        place = np.arange(self.groups * self.half_k)
        index = np.arange(self.dests)[:, None] * self.width_k + np.minimum(place, self.width_k - 1)[None, :]
        return index.reshape(-1), np.tile(place < self.width_k, self.dests)

    def pairs(self, cosine, sine):
        shape = (self.dests, self.groups, self.half_k, -1)
        both = np.concatenate([cosine.reshape(shape), sine.reshape(shape)], axis=2)
        return both.reshape(self.dests * self.row_k, -1)

    def x_forward(self):
        local = np.arange(LANES)
        cells = (np.arange(self.nx)[:, None] * self.cells_x + local[None, :]).reshape(-1)
        used = np.tile(local < self.span_x, self.nx)
        index, kept = self.index_kx()
        angle = self.angle(index, cells)
        mask = kept[:, None] * used[None, :]
        return constant_halves(self.pairs(np.cos(angle) * mask, -np.sin(angle) * mask))

    def x_inverse(self):
        lane = np.arange(self.pack_x)
        local = lane % self.pad_x
        cells = (np.arange(self.nx)[:, None] * self.cells_x + local[None, :]).reshape(-1)
        used = np.tile((local < self.span_x) & (lane < 3 * self.pad_x), self.nx)
        index, kept = self.index_kx()
        angle = self.angle(index, cells)
        mask = (kept * np.where(index > 0, 2.0, 1.0))[:, None] * used[None, :]
        return constant_halves(self.pairs(np.cos(angle) * mask, -np.sin(angle) * mask))

    def z_tables(self):
        cells = np.arange(self.cells_z)
        tables = []
        for parity in range(self.nz):
            angle = self.angle(self.nz * cells + parity, cells)
            forward = np.concatenate([np.cos(angle).T, np.sin(angle).T], axis=1)
            inverse = np.concatenate([np.cos(angle), np.sin(angle)], axis=1)
            tables += [constant_halves(forward), constant_halves(inverse)]
        return jnp.stack(tables).reshape(self.nz, 2, 2, self.cells_z, 2 * self.cells_z)

    def y_tables(self):
        local = np.arange(self.pad_y)
        cells = (np.arange(self.ny)[:, None] * self.cells_y + local[None, :]).reshape(-1)
        used = np.tile(local < self.span_y, self.ny)
        angle = self.angle(np.arange(GRID), cells)
        cosine, sine = np.cos(angle) * used[None, :], np.sin(angle) * used[None, :]
        forward = constant_halves(np.concatenate([cosine, sine], axis=1))
        inverse = constant_halves(np.concatenate([cosine.T, sine.T], axis=1))
        return forward, inverse

    def green_lines(self):
        index = np.arange(GRID)
        signed = np.where(2 * index < GRID, index, index - GRID)
        square = (signed * signed).astype(np.float32)
        bspline = 36.0 / (4.0 + 2.0 * np.cos(index * (2.0 * np.pi / GRID))) ** 2
        bspline = np.where(2 * index == GRID, 0.0, bspline).astype(np.float32)
        line_x = np.stack([square, bspline])[:, : self.kept]
        line_y = np.stack([square, bspline])[:, :, None]
        line_z = np.stack([square, bspline]).reshape(2, 1, self.cells_z, self.nz)
        line_z = line_z.transpose(3, 0, 1, 2)
        return jnp.asarray(line_x), jnp.asarray(line_y), jnp.asarray(line_z)


def flipped(value, size, mask):
    result, bit = 0, 1
    while bit < size:
        digit = value // bit % 2
        result = result + bit * ((digit + mask // bit % 2) % 2)
        bit *= 2
    return result


class Group:
    def __init__(self, axes, sizes):
        self.axes, self.sizes = axes, sizes
        self.count = int(np.prod(sizes))
        self.steps = sorted(range(1, self.count), key=lambda mask: -bin(mask).count("1"))

    def index(self, coordinates):
        place = 0
        for axis, size in zip(self.axes, self.sizes):
            place = place * size + coordinates[axis]
        return place

    def me(self):
        return self.index({axis: lax.axis_index(axis) for axis in self.axes})

    def partner(self, mask):
        where = {}
        for axis, size in reversed(list(zip(self.axes, self.sizes))):
            where[axis] = flipped(lax.axis_index(axis), size, mask % size)
            mask //= size
        return where

    def copies(self, source, target, send_sems, recv_sems):
        result = []
        for step in self.steps:
            where = self.partner(step)
            result.append(
                pltpu.make_async_remote_copy(
                    src_ref=source(self.index(where)),
                    dst_ref=target(self.me()),
                    send_sem=send_sems(step),
                    recv_sem=recv_sems(step),
                    device_id=where,
                    device_id_type=MESH,
                )
            )
        return result


def greet(groups):
    semaphore = pltpu.get_barrier_semaphore()
    for group in groups:
        for step in group.steps:
            pl.semaphore_signal(
                semaphore, inc=1, device_id=group.partner(step), device_id_type=MESH
            )
    pl.semaphore_wait(semaphore, sum(group.count - 1 for group in groups))


def atoms_kernel(across, along, src_ref, out_ref, send_sems, recv_sems, local_sem):
    mine = across.me() * along.count + along.me()
    greet([across, along])

    def sends(group, source, place, row):
        return group.copies(
            lambda peer: source,
            lambda me: out_ref.at[place],
            lambda step: send_sems.at[row, step],
            lambda step: recv_sems.at[row, step],
        )

    crossing = sends(across, src_ref, mine, 0)
    direct = sends(along, src_ref, mine, 1)
    for copy in crossing + direct:
        copy.start()
    own = pltpu.make_async_copy(src_ref, out_ref.at[mine], local_sem)
    own.start()
    forwarded = []
    for row, (step, copy) in enumerate(zip(across.steps, crossing)):
        copy.wait_recv()
        theirs = across.index(across.partner(step)) * along.count + along.me()
        forwarded += sends(along, out_ref.at[theirs], theirs, 2 + row)
    for copy in forwarded:
        copy.start()
    own.wait()
    for copy in crossing:
        copy.wait_send()
    for copy in direct + forwarded:
        copy.wait()


def shares_kernel(across, along, src_ref, out_ref, sum_ref, first_ref, second_ref, send_sems, recv_sems):
    greet([across, along])
    first = along.copies(
        lambda peer: src_ref.at[peer],
        lambda me: first_ref.at[me],
        lambda step: send_sems.at[0, step],
        lambda step: recv_sems.at[0, step],
    )
    for copy in first:
        copy.start()
    total = src_ref[along.me()]
    for step, copy in zip(along.steps, first):
        copy.wait_recv()
        total = total + first_ref[along.index(along.partner(step))]
    sum_ref[...] = total
    second = across.copies(
        lambda peer: sum_ref.at[peer],
        lambda me: second_ref.at[me],
        lambda step: send_sems.at[1, step],
        lambda step: recv_sems.at[1, step],
    )
    for copy in second:
        copy.start()
    result = sum_ref[across.me()]
    for step, copy in zip(across.steps, second):
        copy.wait_recv()
        result = result + second_ref[across.index(across.partner(step))]
    out_ref[...] = result
    for copy in first + second:
        copy.wait_send()


def group_of(*axes):
    return Group(axes, [lax.axis_size(axis) for axis in axes])


def spline_rows(frac):
    rest = 1.0 - frac
    square = frac * frac
    cube = square * frac
    weights = [
        rest * rest * rest / 6.0,
        (3.0 * cube - 6.0 * square + 4.0) / 6.0,
        (-3.0 * cube + 3.0 * square + 3.0 * frac + 1.0) / 6.0,
        cube / 6.0,
    ]
    slopes = [
        -0.5 * rest * rest,
        1.5 * square - 2.0 * frac,
        -1.5 * square + frac + 0.5,
        0.5 * square,
    ]
    return weights, slopes


def placed(offset, values, dim):
    total = jnp.zeros(offset.shape, jnp.float32)
    for k in range(ORDER):
        total = jnp.where(offset == float(k), values[k][dim : dim + 1], total)
    return total


def offsets(rows, lowest):
    return lax.broadcasted_iota(jnp.int32, (rows, LANES), 0).astype(jnp.float32) - lowest


def fold_sign(parity, part):
    return (1 - 2 * lax.rem(parity * part, 2)).astype(jnp.float32)


def list_units(plan, counts_ref, list_ref):
    place = lax.axis_index("gx")

    def block_step(block, total):
        def listed(octet, begin, end, total):
            def put(chunk, total):
                list_ref[total] = (block * plan.chunks + chunk) * plan.octets + octet
                return total + 1

            return lax.fori_loop(begin, end, put, total)

        ends = 0
        for octet in range(plan.octets):
            start = counts_ref[block, place * plan.octets + octet]
            stop = counts_ref[block, LANES // 2 + place * plan.octets + octet]
            begin = start // LANES
            end = jnp.where(stop > start, (stop + LANES - 1) // LANES, begin)
            if octet == 0:
                ends = jnp.where(stop > start, end, 0)
            total = listed(octet, begin, end, total)
        start = counts_ref[block, plan.nx * plan.octets]
        stop = counts_ref[block, LANES // 2 + plan.nx * plan.octets]
        begin = jnp.maximum(start // LANES, ends)
        end = jnp.where((stop > start) & (place == 0), (stop + LANES - 1) // LANES, begin)
        return listed(0, begin, end, total)

    total = lax.fori_loop(0, plan.blocks, block_step, 0)
    for extra in range(plan.unroll):
        list_ref[total + extra] = 0
    return total


def over_units(plan, counts_ref, list_ref, work):
    total = list_units(plan, counts_ref, list_ref)
    parity = lax.axis_index("gz")

    def step(i, carry):
        for lane in range(plan.unroll):
            unit = i * plan.unroll + lane
            code = list_ref[unit]
            octet = lax.rem(code, plan.octets)
            code = lax.div(code, plan.octets)
            chunk, block = lax.rem(code, plan.chunks), lax.div(code, plan.chunks)
            sign = fold_sign(parity, block // plan.nx)
            work(lane, block, chunk, octet, jnp.where(unit < total, sign, 0.0))
        return carry

    lax.fori_loop(0, (total + plan.unroll - 1) // plan.unroll, step, 0)


def z_offsets(plan, octet, lowest):
    first = lax.axis_index("gx") * plan.window + octet * SUBLANES
    offset = offsets(SUBLANES, lowest - first.astype(jnp.float32))
    wraps = offset < float(ORDER - plan.cells_z)
    factor = jnp.where(wraps, fold_sign(lax.axis_index("gz"), 1), 1.0)
    return jnp.where(wraps, offset + float(plan.cells_z), offset), factor


def spread_kernel(plan, counts_ref, atoms_ref, grid_ref, list_ref, y_ref, x_ref, a_ref):
    grid_ref[...] = jnp.zeros_like(grid_ref)
    x_ref[...] = jnp.zeros_like(x_ref)

    def work(lane, block, chunk, octet, sign):
        atoms = atoms_ref[block, :, pl.ds(pl.multiple_of(chunk * LANES, LANES), LANES)]
        weights, _ = spline_rows(atoms[0:3])
        high, low = halves(
            jnp.concatenate(
                [
                    placed(offsets(plan.pad_x, atoms[4:5]), weights, 0),
                    jnp.zeros((LANES - plan.pad_x, LANES), jnp.float32),
                ],
                axis=0,
            )
        )
        x_ref[lane, :LANES, :LANES] = high
        x_ref[lane, :LANES, LANES:] = high
        x_ref[lane, LANES:, :LANES] = low
        y_ref[lane] = placed(offsets(plan.pad_y, atoms[5:6]), weights, 1)
        offset, factor = z_offsets(plan, octet, atoms[6:7])
        line = placed(offset, weights, 2) * factor * (atoms[3:4] * sign)
        for y in range(0, plan.pad_y, 2):
            pair = jnp.concatenate([y_ref[lane, y : y + 1] * line, y_ref[lane, y + 1 : y + 2] * line], axis=0)
            high, low = halves(pair)
            a_ref[lane, y * SUBLANES : (y + 2) * SUBLANES, :LANES] = high
            a_ref[lane, y * SUBLANES : (y + 2) * SUBLANES, LANES:] = low
        product = mm(a_ref[lane], x_ref[lane], ROWS_BY_ROWS)
        place = pl.ds(pl.multiple_of(lax.rem(block, plan.nx) * LANES, LANES), LANES)
        grid_ref[octet, :, place] += product[:, :LANES] + product[:, LANES:]

    over_units(plan, counts_ref, list_ref, work)


def regroup(plan, values):
    shape = values[0].shape
    group = lax.broadcasted_iota(jnp.int32, shape, 1) // plan.window
    moved = []
    for step in range(plan.nx):
        mixed = values[step % plan.nx]
        for part in range(1, plan.nx):
            mixed = jnp.where(group == part, values[(part + step) % plan.nx], mixed)
        moved.append(pltpu.roll(mixed, step * plan.window, 1) if step else mixed)
    results = []
    for part in range(plan.nx):
        result = moved[(-part) % plan.nx]
        for other in range(1, plan.nx):
            result = jnp.where(group == other, moved[(other - part) % plan.nx], result)
        results.append(result)
    return results


def mesh_kernel(
    plan,
    group,
    grid_ref,
    x_forward_ref,
    z_table_ref,
    y_forward_ref,
    y_inverse_ref,
    line_x_ref,
    line_y_ref,
    line_z_ref,
    x_inverse_ref,
    pot_ref,
    there_out_ref,
    there_in_ref,
    back_out_ref,
    back_in_ref,
    u_ref,
    o_ref,
    mid_ref,
    send_sems,
    recv_sems,
    local_sems,
):
    parity = lax.axis_index("gz")
    device = group.me()
    row_k, nx = plan.row_k, plan.nx
    greet([group])

    def sending(way, kind, part, out_ref, in_ref):
        first, count = part
        lanes = pl.ds(first * LANES, count * LANES)
        rows = pl.ds(kind * SUBLANES, SUBLANES)
        slot = plan.parts.index(part) if part in plan.parts else 0
        copies = group.copies(
            lambda peer: out_ref.at[peer, rows, lanes],
            lambda place: in_ref.at[place, rows, lanes],
            lambda step: send_sems.at[way, kind, slot, step],
            lambda step: recv_sems.at[way, kind, slot, step],
        )
        own = pltpu.make_async_copy(
            out_ref.at[device, rows, lanes],
            in_ref.at[device, rows, lanes],
            local_sems.at[way, kind, slot],
        )
        return copies, own

    def start(copies, own):
        for copy in copies:
            copy.start()
        own.start()

    def arrive(copies, own):
        for copy in copies:
            copy.wait_recv()
        own.wait()

    def tile_lanes(tile):
        return pl.ds(pl.multiple_of(tile * LANES, LANES), LANES)

    def x_forward(tile, carry):
        pieces = []
        for other in range(nx):
            row = pl.multiple_of((tile * nx + other) * SUBLANES, SUBLANES)
            for octet in range(plan.octets):
                pieces.append(grid_ref[octet, pl.ds(row, SUBLANES), :])
        high, low = halves(jnp.concatenate(pieces, axis=0))
        first_pass = mm(x_forward_ref[0], jnp.concatenate([high, low], axis=0), ROWS_BY_ROWS)
        second_pass = mm(x_forward_ref[1], high, ROWS_BY_ROWS)
        total = first_pass[:, :LANES] + (first_pass[:, LANES:] + second_pass)
        there_out_ref[:, :, tile_lanes(tile)] = total.reshape(plan.dests, row_k, LANES)
        return carry

    whole = [(0, plan.tiles)]
    kinds = range(plan.groups)
    there = [
        [sending(0, kind, part, there_out_ref, there_in_ref) for part in (whole if kind else plan.parts)]
        for kind in kinds
    ]
    back = [[sending(1, kind, part, back_out_ref, back_in_ref) for part in plan.parts] for kind in kinds]
    for part, (first, count) in enumerate(plan.parts):
        lax.fori_loop(first, first + count, x_forward, 0)
        start(*there[0][part])
    for kind in kinds[1:]:
        start(*there[kind][0])

    imaginary = lax.broadcasted_iota(jnp.int32, (1, SUBLANES, 1), 1) >= plan.half_k

    def z_transform(direction, rows):
        high = z_table_ref[parity, direction, 0]
        both = jnp.concatenate([high, high], axis=0)
        low = z_table_ref[parity, direction, 1]
        total = mm(u_ref[:rows], both) + mm(u_ref[:rows, :LANES], low)
        total = total.reshape(rows // SUBLANES, SUBLANES, 2 * LANES)
        swapped = pltpu.roll(total[..., LANES:], plan.half_k, 1)
        swapped = jnp.where(imaginary == (direction == 0), -swapped, swapped)
        return (total[..., :LANES] + swapped).reshape(rows, LANES)

    def z_forward(kind, gy):
        rows = slice(kind * SUBLANES, (kind + 1) * SUBLANES)
        for tile in range(plan.tiles):
            here = pl.ds(tile * LANES, LANES)
            values = regroup(plan, [there_in_ref[gy * nx + gx, rows, here] for gx in range(nx)])
            for other in range(0, nx, 2):
                row = (tile * nx + other) * SUBLANES
                high, low = halves(jnp.concatenate(values[other : other + 2], axis=0))
                u_ref[row : row + 2 * SUBLANES, :LANES] = high
                u_ref[row : row + 2 * SUBLANES, LANES:] = low
        row = pl.multiple_of(gy * plan.rows, SUBLANES)
        mid_ref[kind, pl.ds(row, plan.rows), :] = z_transform(0, plan.rows)

    def column(kind, j):
        lines = [pl.ds(j + half * plan.half_k, plan.all_y, stride=SUBLANES) for half in range(2)]
        real = mid_ref[kind, lines[0], :]
        imag = mid_ref[kind, lines[1], :]
        stacked = jnp.concatenate(
            [jnp.concatenate([real, imag], axis=1), jnp.concatenate([imag, -real], axis=1)], axis=0
        )
        high, low = halves(stacked)
        spectrum = mm(y_forward_ref[0], high) + (mm(y_forward_ref[0], low) + mm(y_forward_ref[1], high))
        kx = device * plan.width_k + kind * plan.half_k + j
        square = (line_y_ref[0] + line_z_ref[parity, 0]) + line_x_ref[0, kx]
        factor = (line_y_ref[1] * line_z_ref[parity, 1]) * line_x_ref[1, kx]
        green = jnp.where(
            square > 0.0,
            coulomb
            * jnp.exp(square * (-np.pi**2 / (ewald * ewald * GRID * GRID)))
            * factor
            / (np.pi * GRID * jnp.maximum(square, 1.0)),
            0.0,
        )
        real = spectrum[:, :LANES] * green
        imag = spectrum[:, LANES:] * green
        stacked = jnp.concatenate(
            [jnp.concatenate([real, imag], axis=1), jnp.concatenate([-imag, real], axis=1)], axis=0
        )
        high, low = halves(stacked)
        result = mm(y_inverse_ref[0], high) + (mm(y_inverse_ref[0], low) + mm(y_inverse_ref[1], high))
        return lines, result

    def columns(kind, i):
        results = [column(kind, i * 2 + other) for other in range(2)]
        for lines, result in results:
            mid_ref[kind, lines[0], :] = result[:, :LANES]
            mid_ref[kind, lines[1], :] = result[:, LANES:]

    def z_backward(kind, part, gy):
        first, count = part
        size = count * nx * SUBLANES
        row = pl.multiple_of(gy * plan.rows + first * nx * SUBLANES, SUBLANES)
        high, low = halves(mid_ref[kind, pl.ds(row, size), :])
        u_ref[:size, :LANES] = high
        u_ref[:size, LANES:] = low
        o_ref[:size] = z_transform(1, size)
        for tile in range(count):
            values = []
            for other in range(nx):
                row = (tile * nx + other) * SUBLANES
                values.append(o_ref[row : row + SUBLANES])
            here = pl.ds((first + tile) * LANES, LANES)
            rows = slice(kind * SUBLANES, (kind + 1) * SUBLANES)
            for gx, value in enumerate(regroup(plan, values)):
                back_out_ref[gy * nx + gx, rows, here] = value

    def each(count, work, *fixed):
        def step(i, carry):
            work(*fixed, i)
            return carry

        lax.fori_loop(0, count, step, 0)

    for kind in kinds:
        for piece in there[kind]:
            arrive(*piece)
        each(plan.ny, z_forward, kind)
        each(min(plan.half_k, plan.width_k) // 2, columns, kind)
        for part, piece in zip(plan.parts, back[kind]):
            each(plan.ny, z_backward, kind, part)
            start(*piece)

    def x_inverse(tile, carry):
        lines = back_in_ref[:, :, tile_lanes(tile)].reshape(plan.dests * row_k, LANES)
        high, low = halves(lines.T)
        first_pass = mm(jnp.concatenate([high, low], axis=0), x_inverse_ref[0])
        value = first_pass[:LANES] + (first_pass[LANES:] + mm(high, x_inverse_ref[1]))
        lane = lax.rem(lax.broadcasted_iota(jnp.int32, value.shape, 1), plan.pack_x)
        rest = value - value.astype(jnp.bfloat16).astype(jnp.float32)
        value = jnp.where((lane >= plan.pad_x) & (lane < 2 * plan.pad_x), rest, value)
        for octet in range(plan.octets):
            for other in range(0, nx, 2):
                pieces = []
                for extra in range(2):
                    row = (other + extra) * plan.window + octet * SUBLANES
                    pieces.append(value[row : row + SUBLANES])
                row = pl.multiple_of((tile * nx + other) * SUBLANES, 2 * SUBLANES)
                pot_ref[octet, pl.ds(row, 2 * SUBLANES), :] = jnp.concatenate(pieces, axis=0).astype(jnp.bfloat16)
        return carry

    for part, (first, count) in enumerate(plan.parts):
        for kind in kinds:
            arrive(*back[kind][part])
        lax.fori_loop(first, first + count, x_inverse, 0)
    for pieces in there + back:
        for copies, _ in pieces:
            for copy in copies:
                copy.wait_send()


def gather_kernel(plan, counts_ref, atoms_ref, pot_ref, out_ref, list_ref, y_ref, x_ref, p_ref):
    out_ref[...] = jnp.zeros_like(out_ref)
    pack = plan.pack_x

    def work(lane, block, chunk, octet, sign):
        atoms = atoms_ref[block, :, pl.ds(pl.multiple_of(chunk * LANES, LANES), LANES)]
        weights, slopes = spline_rows(atoms[0:3])
        offset = offsets(plan.pad_x, atoms[4:5])
        table = jnp.concatenate([placed(offset, weights, 0), placed(offset, slopes, 0)], axis=1)
        high = table.astype(jnp.bfloat16).astype(jnp.float32)
        unused = jnp.zeros((pack - 3 * plan.pad_x, 2 * LANES), jnp.float32)
        x_ref[lane] = jnp.concatenate([high, high, table - high, unused], axis=0).astype(jnp.bfloat16)
        offset = offsets(plan.pad_y, atoms[5:6])
        y_ref[lane, 0] = placed(offset, weights, 1)
        y_ref[lane, 1] = placed(offset, slopes, 1)
        offset, factor = z_offsets(plan, octet, atoms[6:7])
        factor = factor * sign
        weight_z = placed(offset, weights, 2) * factor
        slope_z = placed(offset, slopes, 2) * factor
        place = pl.ds(pl.multiple_of(lax.rem(block, plan.nx) * pack, LANES), pack)
        p_ref[lane] = mm(pot_ref[octet, :, place], x_ref[lane])
        total_x = jnp.zeros((SUBLANES, LANES), jnp.float32)
        total_y = jnp.zeros((SUBLANES, LANES), jnp.float32)
        total_z = jnp.zeros((SUBLANES, LANES), jnp.float32)
        for y in range(plan.pad_y):
            rows = slice(y * SUBLANES, (y + 1) * SUBLANES)
            plain = p_ref[lane, rows, :LANES]
            weight = y_ref[lane, 0, y : y + 1]
            total_x += weight * p_ref[lane, rows, LANES:]
            total_y += y_ref[lane, 1, y : y + 1] * plain
            total_z += weight * plain
        totals = [weight_z * total_x, weight_z * total_y, slope_z * total_z]
        for dim in range(3):
            row = jnp.sum(totals[dim], axis=0, keepdims=True)
            out_ref[lax.rem(block, plan.nx), block // plan.nx, pl.ds(dim * plan.chunks + chunk, 1), :] += row

    over_units(plan, counts_ref, list_ref, work)


def vmem_call(kernel, out_shape, scratch_shapes, smem=(), **params):
    def call(*operands):
        specs = [
            pl.BlockSpec(memory_space=pltpu.SMEM if i in smem else pltpu.VMEM)
            for i in range(len(operands))
        ]
        return pl.pallas_call(
            kernel,
            in_specs=specs,
            out_specs=pl.BlockSpec(memory_space=pltpu.VMEM),
            out_shape=out_shape,
            scratch_shapes=scratch_shapes,
            compiler_params=pltpu.CompilerParams(vmem_limit_bytes=50 * 2**20, **params),
        )(*operands)

    return call


def per_device(charges, fractions, base_cells, counts):
    capacity = charges.shape[0]
    plan = Plan(lax.axis_size("gz"), lax.axis_size("gy"), lax.axis_size("gx"), capacity)
    f32, bf16 = jnp.float32, jnp.bfloat16
    slot = jnp.arange(capacity, dtype=jnp.int32)
    live = slot < counts.reshape(())
    charge = jnp.where(live, charges, jnp.zeros_like(charges))
    local_x = (base_cells[0] - lax.axis_index("gx") * plan.cells_x).astype(f32)
    local_y = (base_cells[1] - lax.axis_index("gy") * plan.cells_y).astype(f32)
    key = jnp.where(live, base_cells[2] - lax.axis_index("gz") * plan.cells_z, plan.cells_z)
    key, slot, t_x, t_y, t_z, charge, local_x, local_y = lax.sort(
        [key, slot, fractions[0], fractions[1], fractions[2], charge, local_x, local_y],
        num_keys=1,
        is_stable=False,
    )
    edges = np.full(LANES, -1)
    starts = np.arange(plan.nx * plan.octets + 1) * SUBLANES
    edges[: len(starts)] = starts - plan.halo
    edges[LANES // 2 : LANES // 2 + len(starts)] = np.minimum(starts + SUBLANES, plan.cells_z)
    counted = jnp.sum((key[None, :] < jnp.asarray(edges)[:, None]).astype(f32), axis=1)
    counted = jnp.pad(counted, (0, capacity - LANES))
    atoms = jnp.stack([t_x, t_y, t_z, charge, local_x, local_y, key.astype(f32), counted])
    across, along = group_of("gz"), group_of("gx")
    most = max(plan.nz, plan.nx)
    atoms = vmem_call(
        functools.partial(atoms_kernel, across, along),
        jax.ShapeDtypeStruct((plan.blocks,) + atoms.shape, f32),
        [
            pltpu.SemaphoreType.DMA((plan.nz + 1, most)),
            pltpu.SemaphoreType.DMA((plan.nz + 1, most)),
            pltpu.SemaphoreType.DMA,
        ],
        collective_id=0,
        has_side_effects=True,
    )(atoms)
    counts = atoms[:, 7, :LANES].astype(jnp.int32)

    lanes = plan.tiles * LANES
    mesh_shape = (plan.octets, plan.rows, plan.nx * LANES)
    units = plan.blocks * plan.chunks * plan.octets + plan.unroll
    grid = vmem_call(
        functools.partial(spread_kernel, plan),
        jax.ShapeDtypeStruct(mesh_shape, f32),
        [
            pltpu.SMEM((units,), jnp.int32),
            pltpu.VMEM((plan.unroll, plan.pad_y, LANES), f32),
            pltpu.VMEM((plan.unroll, 2 * LANES, 2 * LANES), bf16),
            pltpu.VMEM((plan.unroll, plan.rows, 2 * LANES), bf16),
        ],
        smem=(0,),
    )(counts, atoms)
    y_forward, y_inverse = plan.y_tables()
    line_x, line_y, line_z = plan.green_lines()
    group = group_of("gy", "gx")
    parts = len(plan.parts)
    half = pltpu.VMEM((plan.dests, plan.row_k, lanes), f32)
    potential = vmem_call(
        functools.partial(mesh_kernel, plan, group),
        jax.ShapeDtypeStruct((plan.octets, plan.rows, plan.nx * plan.pack_x), bf16),
        [
            half,
            half,
            half,
            half,
            pltpu.VMEM((plan.rows, 2 * LANES), bf16),
            pltpu.VMEM((plan.rows, LANES), f32),
            pltpu.VMEM((plan.groups, plan.all_y * SUBLANES, LANES), f32),
            pltpu.SemaphoreType.DMA((2, plan.groups, parts, group.count)),
            pltpu.SemaphoreType.DMA((2, plan.groups, parts, group.count)),
            pltpu.SemaphoreType.DMA((2, plan.groups, parts)),
        ],
        smem=(5,),
        collective_id=1,
        has_side_effects=True,
    )(
        grid,
        plan.x_forward(),
        plan.z_tables(),
        y_forward,
        y_inverse,
        line_x,
        line_y,
        line_z,
        plan.x_inverse(),
    )
    shares = vmem_call(
        functools.partial(gather_kernel, plan),
        jax.ShapeDtypeStruct((plan.nx, plan.nz, 3 * plan.chunks, LANES), f32),
        [
            pltpu.SMEM((units,), jnp.int32),
            pltpu.VMEM((plan.unroll, 2, plan.pad_y, LANES), f32),
            pltpu.VMEM((plan.unroll, plan.pack_x, 2 * LANES), bf16),
            pltpu.VMEM((plan.unroll, plan.rows, 2 * LANES), f32),
        ],
        smem=(0,),
    )(counts, atoms, potential)
    share = shares.shape[2:]
    total = vmem_call(
        functools.partial(shares_kernel, across, along),
        jax.ShapeDtypeStruct(share, f32),
        [
            pltpu.VMEM((plan.nz,) + share, f32),
            pltpu.VMEM(shares.shape, f32),
            pltpu.VMEM((plan.nz,) + share, f32),
            pltpu.SemaphoreType.DMA((2, most)),
            pltpu.SemaphoreType.DMA((2, most)),
        ],
        collective_id=2,
        has_side_effects=True,
    )(shares)
    forces = -charge[None, :] * total.reshape(3, capacity)
    result = lax.sort([slot, forces[0], forces[1], forces[2]], num_keys=1, is_stable=False)
    return jnp.stack(result[1:])


def solution(mesh):
    in_specs = (
        P(("gz", "gy", "gx")),
        P(None, ("gz", "gy", "gx")),
        P(None, ("gz", "gy", "gx")),
        P("gz", "gy", "gx"),
    )
    out_specs = P(None, ("gz", "gy", "gx"))
    return jax.shard_map(
        per_device, mesh=mesh, in_specs=in_specs, out_specs=out_specs, check_vma=False
    )
```

```python
import functools

import jax
import jax.numpy as jnp
import numpy as np
from jax import lax
from jax.experimental import pallas as pl
from jax.experimental.pallas import tpu as pltpu
from jax.sharding import PartitionSpec as P

GRID = 256
ORDER = 4
LANES = 128
SUBLANES = 8

coulomb = 332.0636
ewald = 0.7
MESH = pl.DeviceIdType.MESH
ROWS_BY_ROWS = (((1,), (1,)), ((), ()))


def round_up(value, unit):
    return -(-value // unit) * unit


def halves(value):
    high = value.astype(jnp.bfloat16)
    low = (value - high.astype(jnp.float32)).astype(jnp.bfloat16)
    return high, low


def constant_halves(value):
    value = np.asarray(value, np.float32)
    high = value.astype(jnp.bfloat16)
    low = (value - high.astype(np.float32)).astype(jnp.bfloat16)
    return jnp.asarray(np.stack([high, low]))


def mm(a, b, contract=(((1,), (0,)), ((), ()))):
    return lax.dot_general(a, b, contract, preferred_element_type=jnp.float32)


class Plan:
    def __init__(self, nz, ny, nx, capacity):
        self.nz, self.ny, self.nx = nz, ny, nx
        self.capacity = capacity
        self.chunks = capacity // LANES
        self.blocks = nz * nx
        self.cells_x = GRID // nx
        self.cells_y = GRID // ny
        self.cells_z = GRID // nz
        self.halo = ORDER - 1
        self.span_x = self.cells_x + self.halo
        self.span_y = self.cells_y + self.halo
        self.window = self.cells_z // nx
        self.octets = self.window // SUBLANES
        self.tiles = -(-self.span_y // nx)
        self.pad_y = self.tiles * nx
        self.rows = self.pad_y * SUBLANES
        self.dests = ny * nx
        self.kept = GRID // 2
        self.width_k = self.kept // self.dests
        self.half_k = SUBLANES // 2
        self.groups = -(-self.width_k // self.half_k)
        self.row_k = self.groups * SUBLANES
        self.all_y = ny * self.pad_y
        self.pad_x = round_up(self.span_x, SUBLANES)
        self.pack_x = round_up(3 * self.pad_x, LANES)
        self.unroll = 4
        edges = np.round(self.tiles * np.array([0.0, 0.12, 0.36, 0.66, 1.0])).astype(int)
        sizes = [int(size) for size in np.diff(edges)]
        self.parts = [(sum(sizes[:i]), size) for i, size in enumerate(sizes)]
        sizes = sizes[::-1]
        self.back_parts = [(sum(sizes[:i]), size) for i, size in enumerate(sizes)]
        assert nz == 2 and self.cells_z == LANES and self.span_x <= LANES

    def angle(self, outputs, inputs):
        return (outputs[:, None] * inputs[None, :] % GRID) * (2.0 * np.pi / GRID)

    def index_kx(self):
        place = np.arange(self.groups * self.half_k)
        index = np.arange(self.dests)[:, None] * self.width_k + np.minimum(place, self.width_k - 1)[None, :]
        return index.reshape(-1), np.tile(place < self.width_k, self.dests)

    def pairs(self, cosine, sine):
        shape = (self.dests, self.groups, self.half_k, -1)
        both = np.concatenate([cosine.reshape(shape), sine.reshape(shape)], axis=2)
        return both.reshape(self.dests * self.row_k, -1)

    def x_forward(self):
        local = np.arange(LANES)
        cells = (np.arange(self.nx)[:, None] * self.cells_x + local[None, :]).reshape(-1)
        used = np.tile(local < self.span_x, self.nx)
        index, kept = self.index_kx()
        angle = self.angle(index, cells)
        mask = kept[:, None] * used[None, :]
        return constant_halves(self.pairs(np.cos(angle) * mask, -np.sin(angle) * mask))

    def x_inverse(self):
        lane = np.arange(self.pack_x)
        local = lane % self.pad_x
        cells = (np.arange(self.nx)[:, None] * self.cells_x + local[None, :]).reshape(-1)
        used = np.tile((local < self.span_x) & (lane < 3 * self.pad_x), self.nx)
        index, kept = self.index_kx()
        angle = self.angle(index, cells)
        mask = (kept * np.where(index > 0, 2.0, 1.0))[:, None] * used[None, :]
        return constant_halves(self.pairs(np.cos(angle) * mask, -np.sin(angle) * mask))

    def z_tables(self):
        cells = np.arange(self.cells_z)
        tables = []
        for parity in range(self.nz):
            angle = self.angle(self.nz * cells + parity, cells)
            forward = np.concatenate([np.cos(angle).T, np.sin(angle).T], axis=1)
            inverse = np.concatenate([np.cos(angle), np.sin(angle)], axis=1)
            tables += [constant_halves(forward), constant_halves(inverse)]
        return jnp.stack(tables).reshape(self.nz, 2, 2, self.cells_z, 2 * self.cells_z)

    def y_tables(self):
        local = np.arange(self.pad_y)
        cells = (np.arange(self.ny)[:, None] * self.cells_y + local[None, :]).reshape(-1)
        used = np.tile(local < self.span_y, self.ny)
        angle = self.angle(np.arange(GRID), cells)
        cosine, sine = np.cos(angle) * used[None, :], np.sin(angle) * used[None, :]
        forward = constant_halves(np.concatenate([cosine, sine], axis=1))
        inverse = constant_halves(np.concatenate([cosine.T, sine.T], axis=1))
        return forward, inverse

    def green_lines(self):
        index = np.arange(GRID)
        signed = np.where(2 * index < GRID, index, index - GRID)
        square = (signed * signed).astype(np.float32)
        bspline = 36.0 / (4.0 + 2.0 * np.cos(index * (2.0 * np.pi / GRID))) ** 2
        bspline = np.where(2 * index == GRID, 0.0, bspline).astype(np.float32)
        line_x = np.stack([square, bspline])[:, : self.kept]
        line_y = np.stack([square, bspline])[:, :, None]
        line_z = np.stack([square, bspline]).reshape(2, 1, self.cells_z, self.nz)
        line_z = line_z.transpose(3, 0, 1, 2)
        return jnp.asarray(line_x), jnp.asarray(line_y), jnp.asarray(line_z)


def flipped(value, size, mask):
    result, bit = 0, 1
    while bit < size:
        digit = value // bit % 2
        result = result + bit * ((digit + mask // bit % 2) % 2)
        bit *= 2
    return result


class Group:
    def __init__(self, axes, sizes):
        self.axes, self.sizes = axes, sizes
        self.count = int(np.prod(sizes))
        self.steps = sorted(range(1, self.count), key=lambda mask: -bin(mask).count("1"))

    def index(self, coordinates):
        place = 0
        for axis, size in zip(self.axes, self.sizes):
            place = place * size + coordinates[axis]
        return place

    def me(self):
        return self.index({axis: lax.axis_index(axis) for axis in self.axes})

    def partner(self, mask):
        where = {}
        for axis, size in reversed(list(zip(self.axes, self.sizes))):
            where[axis] = flipped(lax.axis_index(axis), size, mask % size)
            mask //= size
        return where

    def copies(self, source, target, send_sems, recv_sems):
        result = []
        for step in self.steps:
            where = self.partner(step)
            result.append(
                pltpu.make_async_remote_copy(
                    src_ref=source(self.index(where)),
                    dst_ref=target(self.me()),
                    send_sem=send_sems(step),
                    recv_sem=recv_sems(step),
                    device_id=where,
                    device_id_type=MESH,
                )
            )
        return result


def greet(groups):
    semaphore = pltpu.get_barrier_semaphore()
    for group in groups:
        for step in group.steps:
            pl.semaphore_signal(
                semaphore, inc=1, device_id=group.partner(step), device_id_type=MESH
            )
    pl.semaphore_wait(semaphore, sum(group.count - 1 for group in groups))


def atoms_kernel(across, along, pieces, src_ref, out_ref, send_sems, recv_sems, local_sem):
    mine = across.me() * along.count + along.me()
    greet([across, along])
    width = src_ref.shape[1] // pieces
    lanes = [pl.ds(piece * width, width) for piece in range(pieces)]

    def sends(group, source, place, row, piece):
        return group.copies(
            lambda peer: source.at[:, lanes[piece]],
            lambda me: out_ref.at[place, :, lanes[piece]],
            lambda step: send_sems.at[row, piece, step],
            lambda step: recv_sems.at[row, piece, step],
        )

    crossing = [sends(across, src_ref, mine, 0, piece) for piece in range(pieces)]
    direct = [sends(along, src_ref, mine, 1, piece) for piece in range(pieces)]
    for copies in crossing + direct:
        for copy in copies:
            copy.start()
    own = pltpu.make_async_copy(src_ref, out_ref.at[mine], local_sem)
    own.start()
    forwarded = []
    for piece in range(pieces):
        for row, (step, copy) in enumerate(zip(across.steps, crossing[piece])):
            copy.wait_recv()
            theirs = across.index(across.partner(step)) * along.count + along.me()
            copies = sends(along, out_ref.at[theirs], theirs, 2 + row, piece)
            for copy in copies:
                copy.start()
            forwarded.append(copies)
    own.wait()
    for copies in crossing:
        for copy in copies:
            copy.wait_send()
    for copies in direct + forwarded:
        for copy in copies:
            copy.wait()


def shares_kernel(across, along, src_ref, out_ref, sum_ref, first_ref, second_ref, send_sems, recv_sems):
    greet([across, along])
    first = along.copies(
        lambda peer: src_ref.at[peer],
        lambda me: first_ref.at[me],
        lambda step: send_sems.at[0, step],
        lambda step: recv_sems.at[0, step],
    )
    for copy in first:
        copy.start()
    total = src_ref[along.me()]
    for step, copy in zip(along.steps, first):
        copy.wait_recv()
        total = total + first_ref[along.index(along.partner(step))]
    sum_ref[...] = total
    second = across.copies(
        lambda peer: sum_ref.at[peer],
        lambda me: second_ref.at[me],
        lambda step: send_sems.at[1, step],
        lambda step: recv_sems.at[1, step],
    )
    for copy in second:
        copy.start()
    result = sum_ref[across.me()]
    for step, copy in zip(across.steps, second):
        copy.wait_recv()
        result = result + second_ref[across.index(across.partner(step))]
    out_ref[...] = result
    for copy in first + second:
        copy.wait_send()


def group_of(*axes):
    return Group(axes, [lax.axis_size(axis) for axis in axes])


def spline_rows(frac):
    rest = 1.0 - frac
    square = frac * frac
    cube = square * frac
    weights = [
        rest * rest * rest / 6.0,
        (3.0 * cube - 6.0 * square + 4.0) / 6.0,
        (-3.0 * cube + 3.0 * square + 3.0 * frac + 1.0) / 6.0,
        cube / 6.0,
    ]
    slopes = [
        -0.5 * rest * rest,
        1.5 * square - 2.0 * frac,
        -1.5 * square + frac + 0.5,
        0.5 * square,
    ]
    return weights, slopes


def placed(offset, values, dim):
    total = jnp.zeros(offset.shape, jnp.float32)
    for k in range(ORDER):
        total = jnp.where(offset == float(k), values[k][dim : dim + 1], total)
    return total


def offsets(rows, lowest):
    return lax.broadcasted_iota(jnp.int32, (rows, LANES), 0).astype(jnp.float32) - lowest


def fold_sign(parity, part):
    return (1 - 2 * lax.rem(parity * part, 2)).astype(jnp.float32)


def list_units(plan, counts_ref, list_ref):
    place = lax.axis_index("gx")

    def block_step(block, total):
        def listed(octet, begin, end, total):
            def put(chunk, total):
                list_ref[total] = (block * plan.chunks + chunk) * plan.octets + octet
                return total + 1

            return lax.fori_loop(begin, end, put, total)

        ends = 0
        for octet in range(plan.octets):
            start = counts_ref[block, place * plan.octets + octet]
            stop = counts_ref[block, LANES // 2 + place * plan.octets + octet]
            begin = start // LANES
            end = jnp.where(stop > start, (stop + LANES - 1) // LANES, begin)
            if octet == 0:
                ends = jnp.where(stop > start, end, 0)
            total = listed(octet, begin, end, total)
        start = counts_ref[block, plan.nx * plan.octets]
        stop = counts_ref[block, LANES // 2 + plan.nx * plan.octets]
        begin = jnp.maximum(start // LANES, ends)
        end = jnp.where((stop > start) & (place == 0), (stop + LANES - 1) // LANES, begin)
        return listed(0, begin, end, total)

    total = lax.fori_loop(0, plan.blocks, block_step, 0)
    for extra in range(plan.unroll):
        list_ref[total + extra] = 0
    return total


def over_units(plan, counts_ref, list_ref, work):
    total = list_units(plan, counts_ref, list_ref)
    parity = lax.axis_index("gz")

    def step(i, carry):
        for lane in range(plan.unroll):
            unit = i * plan.unroll + lane
            code = list_ref[unit]
            octet = lax.rem(code, plan.octets)
            code = lax.div(code, plan.octets)
            chunk, block = lax.rem(code, plan.chunks), lax.div(code, plan.chunks)
            sign = fold_sign(parity, block // plan.nx)
            work(lane, block, chunk, octet, jnp.where(unit < total, sign, 0.0))
        return carry

    lax.fori_loop(0, (total + plan.unroll - 1) // plan.unroll, step, 0)


def z_offsets(plan, octet, lowest):
    first = lax.axis_index("gx") * plan.window + octet * SUBLANES
    offset = offsets(SUBLANES, lowest - first.astype(jnp.float32))
    wraps = offset < float(ORDER - plan.cells_z)
    factor = jnp.where(wraps, fold_sign(lax.axis_index("gz"), 1), 1.0)
    return jnp.where(wraps, offset + float(plan.cells_z), offset), factor


def spread_kernel(plan, counts_ref, atoms_ref, grid_ref, list_ref, y_ref, x_ref, a_ref):
    grid_ref[...] = jnp.zeros_like(grid_ref)
    x_ref[...] = jnp.zeros_like(x_ref)

    def work(lane, block, chunk, octet, sign):
        atoms = atoms_ref[block, :, pl.ds(pl.multiple_of(chunk * LANES, LANES), LANES)]
        weights, _ = spline_rows(atoms[0:3])
        high, low = halves(
            jnp.concatenate(
                [
                    placed(offsets(plan.pad_x, atoms[4:5]), weights, 0),
                    jnp.zeros((LANES - plan.pad_x, LANES), jnp.float32),
                ],
                axis=0,
            )
        )
        x_ref[lane, :LANES, :LANES] = high
        x_ref[lane, :LANES, LANES:] = high
        x_ref[lane, LANES:, :LANES] = low
        y_ref[lane] = placed(offsets(plan.pad_y, atoms[5:6]), weights, 1)
        offset, factor = z_offsets(plan, octet, atoms[6:7])
        line = placed(offset, weights, 2) * factor * (atoms[3:4] * sign)
        for y in range(0, plan.pad_y, 2):
            pair = jnp.concatenate([y_ref[lane, y : y + 1] * line, y_ref[lane, y + 1 : y + 2] * line], axis=0)
            high, low = halves(pair)
            a_ref[lane, y * SUBLANES : (y + 2) * SUBLANES, :LANES] = high
            a_ref[lane, y * SUBLANES : (y + 2) * SUBLANES, LANES:] = low
        product = mm(a_ref[lane], x_ref[lane], ROWS_BY_ROWS)
        place = pl.ds(pl.multiple_of(lax.rem(block, plan.nx) * LANES, LANES), LANES)
        grid_ref[octet, :, place] += product[:, :LANES] + product[:, LANES:]

    over_units(plan, counts_ref, list_ref, work)


def regroup(plan, values):
    shape = values[0].shape
    group = lax.broadcasted_iota(jnp.int32, shape, 1) // plan.window
    moved = []
    for step in range(plan.nx):
        mixed = values[step % plan.nx]
        for part in range(1, plan.nx):
            mixed = jnp.where(group == part, values[(part + step) % plan.nx], mixed)
        moved.append(pltpu.roll(mixed, step * plan.window, 1) if step else mixed)
    results = []
    for part in range(plan.nx):
        result = moved[(-part) % plan.nx]
        for other in range(1, plan.nx):
            result = jnp.where(group == other, moved[(other - part) % plan.nx], result)
        results.append(result)
    return results


def mesh_kernel(
    plan,
    group,
    grid_ref,
    x_forward_ref,
    z_table_ref,
    y_forward_ref,
    y_inverse_ref,
    line_x_ref,
    line_y_ref,
    line_z_ref,
    x_inverse_ref,
    pot_ref,
    there_out_ref,
    there_in_ref,
    back_out_ref,
    back_in_ref,
    u_ref,
    o_ref,
    mid_ref,
    send_sems,
    recv_sems,
    local_sems,
):
    parity = lax.axis_index("gz")
    device = group.me()
    row_k, nx = plan.row_k, plan.nx
    greet([group])

    def sending(way, kind, slot, part, out_ref, in_ref):
        first, count = part
        lanes = pl.ds(first * LANES, count * LANES)
        rows = pl.ds(kind * SUBLANES, SUBLANES)
        copies = group.copies(
            lambda peer: out_ref.at[peer, rows, lanes],
            lambda place: in_ref.at[place, rows, lanes],
            lambda step: send_sems.at[way, kind, slot, step],
            lambda step: recv_sems.at[way, kind, slot, step],
        )
        own = pltpu.make_async_copy(
            out_ref.at[device, rows, lanes],
            in_ref.at[device, rows, lanes],
            local_sems.at[way, kind, slot],
        )
        return copies, own

    def start(copies, own):
        for copy in copies:
            copy.start()
        own.start()

    def arrive(copies, own):
        for copy in copies:
            copy.wait_recv()
        own.wait()

    def tile_lanes(tile):
        return pl.ds(pl.multiple_of(tile * LANES, LANES), LANES)

    def x_forward(tile, carry):
        pieces = []
        for other in range(nx):
            row = pl.multiple_of((tile * nx + other) * SUBLANES, SUBLANES)
            for octet in range(plan.octets):
                pieces.append(grid_ref[octet, pl.ds(row, SUBLANES), :])
        high, low = halves(jnp.concatenate(pieces, axis=0))
        first_pass = mm(x_forward_ref[0], jnp.concatenate([high, low], axis=0), ROWS_BY_ROWS)
        second_pass = mm(x_forward_ref[1], high, ROWS_BY_ROWS)
        total = first_pass[:, :LANES] + (first_pass[:, LANES:] + second_pass)
        there_out_ref[:, :, tile_lanes(tile)] = total.reshape(plan.dests, row_k, LANES)
        return carry

    whole = [(0, plan.tiles)]
    kinds = range(plan.groups)
    there = [
        [
            sending(0, kind, slot, part, there_out_ref, there_in_ref)
            for slot, part in enumerate(whole if kind else plan.parts)
        ]
        for kind in kinds
    ]
    back = [
        [sending(1, kind, slot, part, back_out_ref, back_in_ref) for slot, part in enumerate(plan.back_parts)]
        for kind in kinds
    ]
    for part, (first, count) in enumerate(plan.parts):
        lax.fori_loop(first, first + count, x_forward, 0)
        start(*there[0][part])
    for kind in kinds[1:]:
        start(*there[kind][0])

    imaginary = lax.broadcasted_iota(jnp.int32, (1, SUBLANES, 1), 1) >= plan.half_k

    def z_transform(direction, rows):
        high = z_table_ref[parity, direction, 0]
        both = jnp.concatenate([high, high], axis=0)
        low = z_table_ref[parity, direction, 1]
        total = mm(u_ref[:rows], both) + mm(u_ref[:rows, :LANES], low)
        total = total.reshape(rows // SUBLANES, SUBLANES, 2 * LANES)
        swapped = pltpu.roll(total[..., LANES:], plan.half_k, 1)
        swapped = jnp.where(imaginary == (direction == 0), -swapped, swapped)
        return (total[..., :LANES] + swapped).reshape(rows, LANES)

    def z_forward(kind, gy):
        rows = slice(kind * SUBLANES, (kind + 1) * SUBLANES)
        for tile in range(plan.tiles):
            here = pl.ds(tile * LANES, LANES)
            values = regroup(plan, [there_in_ref[gy * nx + gx, rows, here] for gx in range(nx)])
            for other in range(0, nx, 2):
                row = (tile * nx + other) * SUBLANES
                high, low = halves(jnp.concatenate(values[other : other + 2], axis=0))
                u_ref[row : row + 2 * SUBLANES, :LANES] = high
                u_ref[row : row + 2 * SUBLANES, LANES:] = low
        row = pl.multiple_of(gy * plan.rows, SUBLANES)
        mid_ref[kind, pl.ds(row, plan.rows), :] = z_transform(0, plan.rows)

    def column(kind, j):
        lines = [pl.ds(j + half * plan.half_k, plan.all_y, stride=SUBLANES) for half in range(2)]
        real = mid_ref[kind, lines[0], :]
        imag = mid_ref[kind, lines[1], :]
        stacked = jnp.concatenate(
            [jnp.concatenate([real, imag], axis=1), jnp.concatenate([imag, -real], axis=1)], axis=0
        )
        high, low = halves(stacked)
        spectrum = mm(y_forward_ref[0], high) + (mm(y_forward_ref[0], low) + mm(y_forward_ref[1], high))
        kx = device * plan.width_k + kind * plan.half_k + j
        square = (line_y_ref[0] + line_z_ref[parity, 0]) + line_x_ref[0, kx]
        factor = (line_y_ref[1] * line_z_ref[parity, 1]) * line_x_ref[1, kx]
        green = jnp.where(
            square > 0.0,
            coulomb
            * jnp.exp(square * (-np.pi**2 / (ewald * ewald * GRID * GRID)))
            * factor
            / (np.pi * GRID * jnp.maximum(square, 1.0)),
            0.0,
        )
        real = spectrum[:, :LANES] * green
        imag = spectrum[:, LANES:] * green
        stacked = jnp.concatenate(
            [jnp.concatenate([real, imag], axis=1), jnp.concatenate([-imag, real], axis=1)], axis=0
        )
        high, low = halves(stacked)
        result = mm(y_inverse_ref[0], high) + (mm(y_inverse_ref[0], low) + mm(y_inverse_ref[1], high))
        return lines, result

    def columns(kind, i):
        results = [column(kind, i * 2 + other) for other in range(2)]
        for lines, result in results:
            mid_ref[kind, lines[0], :] = result[:, :LANES]
            mid_ref[kind, lines[1], :] = result[:, LANES:]

    def z_backward(kind, part, gy):
        first, count = part
        size = count * nx * SUBLANES
        row = pl.multiple_of(gy * plan.rows + first * nx * SUBLANES, SUBLANES)
        high, low = halves(mid_ref[kind, pl.ds(row, size), :])
        u_ref[:size, :LANES] = high
        u_ref[:size, LANES:] = low
        o_ref[:size] = z_transform(1, size)
        for tile in range(count):
            values = []
            for other in range(nx):
                row = (tile * nx + other) * SUBLANES
                values.append(o_ref[row : row + SUBLANES])
            here = pl.ds((first + tile) * LANES, LANES)
            rows = slice(kind * SUBLANES, (kind + 1) * SUBLANES)
            for gx, value in enumerate(regroup(plan, values)):
                back_out_ref[gy * nx + gx, rows, here] = value

    def each(count, work, *fixed):
        def step(i, carry):
            work(*fixed, i)
            return carry

        lax.fori_loop(0, count, step, 0)

    for kind in kinds:
        for piece in there[kind]:
            arrive(*piece)
        each(plan.ny, z_forward, kind)
        each(min(plan.half_k, plan.width_k) // 2, columns, kind)
        for part, piece in zip(plan.back_parts, back[kind]):
            each(plan.ny, z_backward, kind, part)
            start(*piece)

    def x_inverse(tile, carry):
        lines = back_in_ref[:, :, tile_lanes(tile)].reshape(plan.dests * row_k, LANES)
        high, low = halves(lines.T)
        first_pass = mm(jnp.concatenate([high, low], axis=0), x_inverse_ref[0])
        value = first_pass[:LANES] + (first_pass[LANES:] + mm(high, x_inverse_ref[1]))
        lane = lax.rem(lax.broadcasted_iota(jnp.int32, value.shape, 1), plan.pack_x)
        rest = value - value.astype(jnp.bfloat16).astype(jnp.float32)
        value = jnp.where((lane >= plan.pad_x) & (lane < 2 * plan.pad_x), rest, value)
        for octet in range(plan.octets):
            for other in range(0, nx, 2):
                pieces = []
                for extra in range(2):
                    row = (other + extra) * plan.window + octet * SUBLANES
                    pieces.append(value[row : row + SUBLANES])
                row = pl.multiple_of((tile * nx + other) * SUBLANES, 2 * SUBLANES)
                pot_ref[octet, pl.ds(row, 2 * SUBLANES), :] = jnp.concatenate(pieces, axis=0).astype(jnp.bfloat16)
        return carry

    for part, (first, count) in enumerate(plan.back_parts):
        for kind in kinds:
            arrive(*back[kind][part])
        lax.fori_loop(first, first + count, x_inverse, 0)
    for pieces in there + back:
        for copies, _ in pieces:
            for copy in copies:
                copy.wait_send()


def gather_kernel(plan, counts_ref, atoms_ref, pot_ref, out_ref, list_ref, y_ref, x_ref, p_ref):
    out_ref[...] = jnp.zeros_like(out_ref)
    pack = plan.pack_x

    def work(lane, block, chunk, octet, sign):
        atoms = atoms_ref[block, :, pl.ds(pl.multiple_of(chunk * LANES, LANES), LANES)]
        weights, slopes = spline_rows(atoms[0:3])
        offset = offsets(plan.pad_x, atoms[4:5])
        table = jnp.concatenate([placed(offset, weights, 0), placed(offset, slopes, 0)], axis=1)
        high = table.astype(jnp.bfloat16).astype(jnp.float32)
        unused = jnp.zeros((pack - 3 * plan.pad_x, 2 * LANES), jnp.float32)
        x_ref[lane] = jnp.concatenate([high, high, table - high, unused], axis=0).astype(jnp.bfloat16)
        offset = offsets(plan.pad_y, atoms[5:6])
        y_ref[lane, 0] = placed(offset, weights, 1)
        y_ref[lane, 1] = placed(offset, slopes, 1)
        offset, factor = z_offsets(plan, octet, atoms[6:7])
        factor = factor * sign
        weight_z = placed(offset, weights, 2) * factor
        slope_z = placed(offset, slopes, 2) * factor
        place = pl.ds(pl.multiple_of(lax.rem(block, plan.nx) * pack, LANES), pack)
        p_ref[lane] = mm(pot_ref[octet, :, place], x_ref[lane])
        total_x = jnp.zeros((SUBLANES, LANES), jnp.float32)
        total_y = jnp.zeros((SUBLANES, LANES), jnp.float32)
        total_z = jnp.zeros((SUBLANES, LANES), jnp.float32)
        for y in range(plan.pad_y):
            rows = slice(y * SUBLANES, (y + 1) * SUBLANES)
            plain = p_ref[lane, rows, :LANES]
            weight = y_ref[lane, 0, y : y + 1]
            total_x += weight * p_ref[lane, rows, LANES:]
            total_y += y_ref[lane, 1, y : y + 1] * plain
            total_z += weight * plain
        totals = [weight_z * total_x, weight_z * total_y, slope_z * total_z]
        for dim in range(3):
            row = jnp.sum(totals[dim], axis=0, keepdims=True)
            out_ref[lax.rem(block, plan.nx), block // plan.nx, pl.ds(dim * plan.chunks + chunk, 1), :] += row

    over_units(plan, counts_ref, list_ref, work)


def vmem_call(kernel, out_shape, scratch_shapes, limit, smem=(), **params):
    def call(*operands):
        specs = [
            pl.BlockSpec(memory_space=pltpu.SMEM if i in smem else pltpu.VMEM)
            for i in range(len(operands))
        ]
        return pl.pallas_call(
            kernel,
            in_specs=specs,
            out_specs=pl.BlockSpec(memory_space=pltpu.VMEM),
            out_shape=out_shape,
            scratch_shapes=scratch_shapes,
            compiler_params=pltpu.CompilerParams(vmem_limit_bytes=limit * 2**20, **params),
        )(*operands)

    return call


def per_device(charges, fractions, base_cells, counts):
    capacity = charges.shape[0]
    plan = Plan(lax.axis_size("gz"), lax.axis_size("gy"), lax.axis_size("gx"), capacity)
    f32, bf16 = jnp.float32, jnp.bfloat16
    slot = jnp.arange(capacity, dtype=jnp.int32)
    live = slot < counts.reshape(())
    charge = jnp.where(live, charges, jnp.zeros_like(charges))
    local_x = (base_cells[0] - lax.axis_index("gx") * plan.cells_x).astype(f32)
    local_y = (base_cells[1] - lax.axis_index("gy") * plan.cells_y).astype(f32)
    key = jnp.where(live, base_cells[2] - lax.axis_index("gz") * plan.cells_z, plan.cells_z)
    key, slot, t_x, t_y, t_z, charge, local_x, local_y = lax.sort(
        [key, slot, fractions[0], fractions[1], fractions[2], charge, local_x, local_y],
        num_keys=1,
        is_stable=False,
    )
    edges = np.full(LANES, -1)
    starts = np.arange(plan.nx * plan.octets + 1) * SUBLANES
    edges[: len(starts)] = starts - plan.halo
    edges[LANES // 2 : LANES // 2 + len(starts)] = np.minimum(starts + SUBLANES, plan.cells_z)
    counted = jnp.sum((key[None, :] < jnp.asarray(edges)[:, None]).astype(f32), axis=1)
    counted = jnp.pad(counted, (0, capacity - LANES))
    atoms = jnp.stack([t_x, t_y, t_z, charge, local_x, local_y, key.astype(f32), counted])
    across, along = group_of("gz"), group_of("gx")
    most = max(plan.nz, plan.nx)
    atoms = vmem_call(
        functools.partial(atoms_kernel, across, along, 2),
        jax.ShapeDtypeStruct((plan.blocks,) + atoms.shape, f32),
        [
            pltpu.SemaphoreType.DMA((plan.nz + 1, 2, most)),
            pltpu.SemaphoreType.DMA((plan.nz + 1, 2, most)),
            pltpu.SemaphoreType.DMA,
        ],
        8,
        collective_id=0,
        has_side_effects=True,
    )(atoms)
    counts = atoms[:, 7, :LANES].astype(jnp.int32)

    lanes = plan.tiles * LANES
    mesh_shape = (plan.octets, plan.rows, plan.nx * LANES)
    units = plan.blocks * plan.chunks * plan.octets + plan.unroll
    grid = vmem_call(
        functools.partial(spread_kernel, plan),
        jax.ShapeDtypeStruct(mesh_shape, f32),
        [
            pltpu.SMEM((units,), jnp.int32),
            pltpu.VMEM((plan.unroll, plan.pad_y, LANES), f32),
            pltpu.VMEM((plan.unroll, 2 * LANES, 2 * LANES), bf16),
            pltpu.VMEM((plan.unroll, plan.rows, 2 * LANES), bf16),
        ],
        16,
        smem=(0,),
    )(counts, atoms)
    y_forward, y_inverse = plan.y_tables()
    line_x, line_y, line_z = plan.green_lines()
    group = group_of("gy", "gx")
    parts = len(plan.parts)
    half = pltpu.VMEM((plan.dests, plan.row_k, lanes), f32)
    potential = vmem_call(
        functools.partial(mesh_kernel, plan, group),
        jax.ShapeDtypeStruct((plan.octets, plan.rows, plan.nx * plan.pack_x), bf16),
        [
            half,
            half,
            half,
            half,
            pltpu.VMEM((plan.rows, 2 * LANES), bf16),
            pltpu.VMEM((plan.rows, LANES), f32),
            pltpu.VMEM((plan.groups, plan.all_y * SUBLANES, LANES), f32),
            pltpu.SemaphoreType.DMA((2, plan.groups, parts, group.count)),
            pltpu.SemaphoreType.DMA((2, plan.groups, parts, group.count)),
            pltpu.SemaphoreType.DMA((2, plan.groups, parts)),
        ],
        28,
        smem=(5,),
        collective_id=1,
        has_side_effects=True,
    )(
        grid,
        plan.x_forward(),
        plan.z_tables(),
        y_forward,
        y_inverse,
        line_x,
        line_y,
        line_z,
        plan.x_inverse(),
    )
    shares = vmem_call(
        functools.partial(gather_kernel, plan),
        jax.ShapeDtypeStruct((plan.nx, plan.nz, 3 * plan.chunks, LANES), f32),
        [
            pltpu.SMEM((units,), jnp.int32),
            pltpu.VMEM((plan.unroll, 2, plan.pad_y, LANES), f32),
            pltpu.VMEM((plan.unroll, plan.pack_x, 2 * LANES), bf16),
            pltpu.VMEM((plan.unroll, plan.rows, 2 * LANES), f32),
        ],
        16,
        smem=(0,),
    )(counts, atoms, potential)
    share = shares.shape[2:]
    total = vmem_call(
        functools.partial(shares_kernel, across, along),
        jax.ShapeDtypeStruct(share, f32),
        [
            pltpu.VMEM((plan.nz,) + share, f32),
            pltpu.VMEM(shares.shape, f32),
            pltpu.VMEM((plan.nz,) + share, f32),
            pltpu.SemaphoreType.DMA((2, most)),
            pltpu.SemaphoreType.DMA((2, most)),
        ],
        8,
        collective_id=2,
        has_side_effects=True,
    )(shares)
    forces = -charge[None, :] * total.reshape(3, capacity)
    result = lax.sort([slot, forces[0], forces[1], forces[2]], num_keys=1, is_stable=False)
    return jnp.stack(result[1:])


def solution(mesh):
    in_specs = (
        P(("gz", "gy", "gx")),
        P(None, ("gz", "gy", "gx")),
        P(None, ("gz", "gy", "gx")),
        P("gz", "gy", "gx"),
    )
    out_specs = P(None, ("gz", "gy", "gx"))
    return jax.shard_map(
        per_device, mesh=mesh, in_specs=in_specs, out_specs=out_specs, check_vma=False
    )
```

```python
import functools

import jax
import jax.numpy as jnp
import numpy as np
from jax import lax
from jax.experimental import pallas as pl
from jax.experimental.pallas import tpu as pltpu
from jax.sharding import PartitionSpec as P

GRID = 256
ORDER = 4
LANES = 128
SUBLANES = 8

coulomb = 332.0636
ewald = 0.7
MESH = pl.DeviceIdType.MESH
ROWS_BY_ROWS = (((1,), (1,)), ((), ()))


def round_up(value, unit):
    return -(-value // unit) * unit


def halves(value):
    high = value.astype(jnp.bfloat16)
    low = (value - high.astype(jnp.float32)).astype(jnp.bfloat16)
    return high, low


def constant_halves(value):
    value = np.asarray(value, np.float32)
    high = value.astype(jnp.bfloat16)
    low = (value - high.astype(np.float32)).astype(jnp.bfloat16)
    return jnp.asarray(np.stack([high, low]))


def mm(a, b, contract=(((1,), (0,)), ((), ()))):
    return lax.dot_general(a, b, contract, preferred_element_type=jnp.float32)


class Plan:
    def __init__(self, nz, ny, nx, capacity):
        self.nz, self.ny, self.nx = nz, ny, nx
        self.capacity = capacity
        self.chunks = capacity // LANES
        self.blocks = nz * nx
        self.cells_x = GRID // nx
        self.cells_y = GRID // ny
        self.cells_z = GRID // nz
        self.halo = ORDER - 1
        self.span_x = self.cells_x + self.halo
        self.span_y = self.cells_y + self.halo
        self.window = self.cells_z // nx
        self.octets = self.window // SUBLANES
        self.tiles = -(-self.span_y // nx)
        self.pad_y = self.tiles * nx
        self.rows = self.pad_y * SUBLANES
        self.dests = ny * nx
        self.kept = GRID // 2
        self.width_k = self.kept // self.dests
        self.half_k = SUBLANES // 2
        self.groups = -(-self.width_k // self.half_k)
        self.row_k = self.groups * SUBLANES
        self.all_y = ny * self.pad_y
        self.pad_x = round_up(self.span_x, SUBLANES)
        self.pack_x = round_up(3 * self.pad_x, LANES)
        self.unroll = 4
        self.pieces = 4
        edges = np.round(self.tiles * np.array([0.0, 0.12, 0.36, 0.66, 1.0])).astype(int)
        sizes = [int(size) for size in np.diff(edges)]
        self.parts = [(sum(sizes[:i]), size) for i, size in enumerate(sizes)]
        sizes = sizes[::-1]
        self.back_parts = [(sum(sizes[:i]), size) for i, size in enumerate(sizes)]
        assert nz == 2 and self.cells_z == LANES and self.span_x <= LANES

    def angle(self, outputs, inputs):
        return (outputs[:, None] * inputs[None, :] % GRID) * (2.0 * np.pi / GRID)

    def index_kx(self):
        place = np.arange(self.groups * self.half_k)
        index = np.arange(self.dests)[:, None] * self.width_k + np.minimum(place, self.width_k - 1)[None, :]
        return index.reshape(-1), np.tile(place < self.width_k, self.dests)

    def pairs(self, cosine, sine):
        shape = (self.dests, self.groups, self.half_k, -1)
        both = np.concatenate([cosine.reshape(shape), sine.reshape(shape)], axis=2)
        return both.reshape(self.dests * self.row_k, -1)

    def x_forward(self):
        local = np.arange(LANES)
        cells = (np.arange(self.nx)[:, None] * self.cells_x + local[None, :]).reshape(-1)
        used = np.tile(local < self.span_x, self.nx)
        index, kept = self.index_kx()
        angle = self.angle(index, cells)
        mask = kept[:, None] * used[None, :]
        return constant_halves(self.pairs(np.cos(angle) * mask, -np.sin(angle) * mask))

    def x_inverse(self):
        lane = np.arange(self.pack_x)
        local = lane % self.pad_x
        cells = (np.arange(self.nx)[:, None] * self.cells_x + local[None, :]).reshape(-1)
        used = np.tile((local < self.span_x) & (lane < 3 * self.pad_x), self.nx)
        index, kept = self.index_kx()
        angle = self.angle(index, cells)
        mask = (kept * np.where(index > 0, 2.0, 1.0))[:, None] * used[None, :]
        return constant_halves(self.pairs(np.cos(angle) * mask, -np.sin(angle) * mask))

    def z_tables(self):
        cells = np.arange(self.cells_z)
        tables = []
        for parity in range(self.nz):
            angle = self.angle(self.nz * cells + parity, cells)
            forward = np.concatenate([np.cos(angle).T, np.sin(angle).T], axis=1)
            inverse = np.concatenate([np.cos(angle), np.sin(angle)], axis=1)
            tables += [constant_halves(forward), constant_halves(inverse)]
        return jnp.stack(tables).reshape(self.nz, 2, 2, self.cells_z, 2 * self.cells_z)

    def y_tables(self):
        local = np.arange(self.pad_y)
        cells = (np.arange(self.ny)[:, None] * self.cells_y + local[None, :]).reshape(-1)
        used = np.tile(local < self.span_y, self.ny)
        angle = self.angle(np.arange(GRID), cells)
        cosine, sine = np.cos(angle) * used[None, :], np.sin(angle) * used[None, :]
        forward = constant_halves(np.concatenate([cosine, sine], axis=1))
        inverse = constant_halves(np.concatenate([cosine.T, sine.T], axis=1))
        return forward, inverse

    def green_lines(self):
        index = np.arange(GRID)
        signed = np.where(2 * index < GRID, index, index - GRID)
        square = (signed * signed).astype(np.float32)
        bspline = 36.0 / (4.0 + 2.0 * np.cos(index * (2.0 * np.pi / GRID))) ** 2
        bspline = np.where(2 * index == GRID, 0.0, bspline).astype(np.float32)
        line_x = np.stack([square, bspline])[:, : self.kept]
        line_y = np.stack([square, bspline])[:, :, None]
        line_z = np.stack([square, bspline]).reshape(2, 1, self.cells_z, self.nz)
        line_z = line_z.transpose(3, 0, 1, 2)
        return jnp.asarray(line_x), jnp.asarray(line_y), jnp.asarray(line_z)


def flipped(value, size, mask):
    result, bit = 0, 1
    while bit < size:
        digit = value // bit % 2
        result = result + bit * ((digit + mask // bit % 2) % 2)
        bit *= 2
    return result


class Group:
    def __init__(self, axes, sizes):
        self.axes, self.sizes = axes, sizes
        self.count = int(np.prod(sizes))
        self.steps = sorted(range(1, self.count), key=lambda mask: -bin(mask).count("1"))

    def index(self, coordinates):
        place = 0
        for axis, size in zip(self.axes, self.sizes):
            place = place * size + coordinates[axis]
        return place

    def me(self):
        return self.index({axis: lax.axis_index(axis) for axis in self.axes})

    def partner(self, mask):
        where = {}
        for axis, size in reversed(list(zip(self.axes, self.sizes))):
            where[axis] = flipped(lax.axis_index(axis), size, mask % size)
            mask //= size
        return where

    def copies(self, source, target, send_sems, recv_sems):
        result = []
        for step in self.steps:
            where = self.partner(step)
            result.append(
                pltpu.make_async_remote_copy(
                    src_ref=source(self.index(where)),
                    dst_ref=target(self.me()),
                    send_sem=send_sems(step),
                    recv_sem=recv_sems(step),
                    device_id=where,
                    device_id_type=MESH,
                )
            )
        return result


def greet(groups, meanwhile=None):
    semaphore = pltpu.get_barrier_semaphore()
    for group in groups:
        for step in group.steps:
            pl.semaphore_signal(
                semaphore, inc=1, device_id=group.partner(step), device_id_type=MESH
            )
    if meanwhile is not None:
        meanwhile()
    pl.semaphore_wait(semaphore, sum(group.count - 1 for group in groups))


def atoms_kernel(across, along, pieces, src_ref, out_ref, send_sems, recv_sems, local_sem):
    mine = across.me() * along.count + along.me()
    greet([across, along])
    width = src_ref.shape[1] // pieces
    lanes = [pl.ds(piece * width, width) for piece in range(pieces)]

    def sends(group, source, place, row, piece):
        return group.copies(
            lambda peer: source.at[:, lanes[piece]],
            lambda me: out_ref.at[place, :, lanes[piece]],
            lambda step: send_sems.at[row, piece, step],
            lambda step: recv_sems.at[row, piece, step],
        )

    crossing = [sends(across, src_ref, mine, 0, piece) for piece in range(pieces)]
    direct = [sends(along, src_ref, mine, 1, piece) for piece in range(pieces)]
    for copies in crossing + direct:
        for copy in copies:
            copy.start()
    own = pltpu.make_async_copy(src_ref, out_ref.at[mine], local_sem)
    own.start()
    forwarded = []
    for piece in range(pieces):
        for row, (step, copy) in enumerate(zip(across.steps, crossing[piece])):
            copy.wait_recv()
            theirs = across.index(across.partner(step)) * along.count + along.me()
            copies = sends(along, out_ref.at[theirs], theirs, 2 + row, piece)
            for copy in copies:
                copy.start()
            forwarded.append(copies)
    own.wait()
    for copies in crossing:
        for copy in copies:
            copy.wait_send()
    for copies in direct + forwarded:
        for copy in copies:
            copy.wait()


def shares_kernel(
    across,
    along,
    src_ref,
    charge_ref,
    slot_ref,
    out_ref,
    sum_ref,
    first_ref,
    second_ref,
    total_ref,
    pick_ref,
    send_sems,
    recv_sems,
):
    chunks = slot_ref.shape[0]
    capacity = chunks * LANES
    slots = jnp.concatenate([slot_ref[...], jnp.zeros((LANES - chunks, LANES), jnp.float32)], axis=0).T

    def pick(chunk):
        wanted = lax.broadcasted_iota(jnp.int32, (LANES, capacity), 1).astype(jnp.float32)
        found = jnp.where(slots[:, chunk : chunk + 1] == wanted, 1.0, 0.0)
        pick_ref[chunk * LANES : (chunk + 1) * LANES, :] = found.astype(jnp.bfloat16)

    half = chunks // 2
    greet([across, along], lambda: [pick(chunk) for chunk in range(half // 2)])
    first = along.copies(
        lambda peer: src_ref.at[peer],
        lambda me: first_ref.at[me],
        lambda step: send_sems.at[0, step],
        lambda step: recv_sems.at[0, step],
    )
    for copy in first:
        copy.start()
    for chunk in range(half // 2, half):
        pick(chunk)
    total = src_ref[along.me()]
    for step, copy in zip(along.steps, first):
        copy.wait_recv()
        total = total + first_ref[along.index(along.partner(step))]
    sum_ref[...] = total
    second = across.copies(
        lambda peer: sum_ref.at[peer],
        lambda me: second_ref.at[me],
        lambda step: send_sems.at[1, step],
        lambda step: recv_sems.at[1, step],
    )
    for copy in second:
        copy.start()
    for chunk in range(half, chunks):
        pick(chunk)
    result = sum_ref[across.me()]
    for step, copy in zip(across.steps, second):
        copy.wait_recv()
        result = result + second_ref[across.index(across.partner(step))]
    charge = charge_ref[...]
    total_ref[...] = -(jnp.concatenate([charge] * 3, axis=0) * result)
    lines = [total_ref[pl.ds(chunk, 3, stride=chunks), :] for chunk in range(chunks)]
    rest = jnp.concatenate(lines, axis=1)
    parts = []
    for _ in range(3):
        part = rest.astype(jnp.bfloat16).astype(jnp.float32)
        rest = rest - part
        parts.append(jnp.concatenate([part, jnp.zeros((SUBLANES - 3, capacity), jnp.float32)], axis=0))
    parts.append(jnp.zeros((SUBLANES, capacity), jnp.float32))
    product = mm(jnp.concatenate(parts, axis=0).astype(jnp.bfloat16), pick_ref[...])
    out_ref[...] = product[0:3] + (product[SUBLANES : SUBLANES + 3] + product[2 * SUBLANES : 2 * SUBLANES + 3])
    for copy in first + second:
        copy.wait_send()


def group_of(*axes):
    return Group(axes, [lax.axis_size(axis) for axis in axes])


def spline_rows(frac):
    rest = 1.0 - frac
    square = frac * frac
    cube = square * frac
    weights = [
        rest * rest * rest / 6.0,
        (3.0 * cube - 6.0 * square + 4.0) / 6.0,
        (-3.0 * cube + 3.0 * square + 3.0 * frac + 1.0) / 6.0,
        cube / 6.0,
    ]
    slopes = [
        -0.5 * rest * rest,
        1.5 * square - 2.0 * frac,
        -1.5 * square + frac + 0.5,
        0.5 * square,
    ]
    return weights, slopes


def placed(offset, values, dim):
    total = jnp.zeros(offset.shape, jnp.float32)
    for k in range(ORDER):
        total = jnp.where(offset == float(k), values[k][dim : dim + 1], total)
    return total


def offsets(rows, lowest):
    return lax.broadcasted_iota(jnp.int32, (rows, LANES), 0).astype(jnp.float32) - lowest


def fold_sign(parity, part):
    return (1 - 2 * lax.rem(parity * part, 2)).astype(jnp.float32)


def list_units(plan, counts_ref, list_ref):
    place = lax.axis_index("gx")

    def block_step(block, total):
        def listed(octet, begin, end, total):
            def put(chunk, total):
                list_ref[total] = (block * plan.chunks + chunk) * plan.octets + octet
                return total + 1

            return lax.fori_loop(begin, end, put, total)

        ends = 0
        for octet in range(plan.octets):
            start = counts_ref[block, place * plan.octets + octet]
            stop = counts_ref[block, LANES // 2 + place * plan.octets + octet]
            begin = start // LANES
            end = jnp.where(stop > start, (stop + LANES - 1) // LANES, begin)
            if octet == 0:
                ends = jnp.where(stop > start, end, 0)
            total = listed(octet, begin, end, total)
        start = counts_ref[block, plan.nx * plan.octets]
        stop = counts_ref[block, LANES // 2 + plan.nx * plan.octets]
        begin = jnp.maximum(start // LANES, ends)
        end = jnp.where((stop > start) & (place == 0), (stop + LANES - 1) // LANES, begin)
        return listed(0, begin, end, total)

    total = lax.fori_loop(0, plan.blocks, block_step, 0)
    for extra in range(plan.unroll):
        list_ref[total + extra] = 0
    return total


def over_units(plan, counts_ref, list_ref, work):
    total = list_units(plan, counts_ref, list_ref)
    parity = lax.axis_index("gz")

    def step(i, carry):
        for lane in range(plan.unroll):
            unit = i * plan.unroll + lane
            code = list_ref[unit]
            octet = lax.rem(code, plan.octets)
            code = lax.div(code, plan.octets)
            chunk, block = lax.rem(code, plan.chunks), lax.div(code, plan.chunks)
            sign = fold_sign(parity, block // plan.nx)
            work(lane, block, chunk, octet, jnp.where(unit < total, sign, 0.0))
        return carry

    lax.fori_loop(0, (total + plan.unroll - 1) // plan.unroll, step, 0)


def z_offsets(plan, octet, lowest):
    first = lax.axis_index("gx") * plan.window + octet * SUBLANES
    offset = offsets(SUBLANES, lowest - first.astype(jnp.float32))
    wraps = offset < float(ORDER - plan.cells_z)
    factor = jnp.where(wraps, fold_sign(lax.axis_index("gz"), 1), 1.0)
    return jnp.where(wraps, offset + float(plan.cells_z), offset), factor


def spread_kernel(plan, counts_ref, atoms_ref, grid_ref, list_ref, y_ref, x_ref, a_ref):
    grid_ref[...] = jnp.zeros_like(grid_ref)
    x_ref[...] = jnp.zeros_like(x_ref)

    def work(lane, block, chunk, octet, sign):
        atoms = atoms_ref[block, :, pl.ds(pl.multiple_of(chunk * LANES, LANES), LANES)]
        weights, _ = spline_rows(atoms[0:3])
        high, low = halves(
            jnp.concatenate(
                [
                    placed(offsets(plan.pad_x, atoms[4:5]), weights, 0),
                    jnp.zeros((LANES - plan.pad_x, LANES), jnp.float32),
                ],
                axis=0,
            )
        )
        x_ref[lane, :LANES, :LANES] = high
        x_ref[lane, :LANES, LANES:] = high
        x_ref[lane, LANES:, :LANES] = low
        y_ref[lane] = placed(offsets(plan.pad_y, atoms[5:6]), weights, 1)
        offset, factor = z_offsets(plan, octet, atoms[6:7])
        line = placed(offset, weights, 2) * factor * (atoms[3:4] * sign)
        for y in range(0, plan.pad_y, 2):
            pair = jnp.concatenate([y_ref[lane, y : y + 1] * line, y_ref[lane, y + 1 : y + 2] * line], axis=0)
            high, low = halves(pair)
            a_ref[lane, y * SUBLANES : (y + 2) * SUBLANES, :LANES] = high
            a_ref[lane, y * SUBLANES : (y + 2) * SUBLANES, LANES:] = low
        product = mm(a_ref[lane], x_ref[lane], ROWS_BY_ROWS)
        place = pl.ds(pl.multiple_of(lax.rem(block, plan.nx) * LANES, LANES), LANES)
        grid_ref[octet, :, place] += product[:, :LANES] + product[:, LANES:]

    over_units(plan, counts_ref, list_ref, work)


def regroup(plan, values):
    shape = values[0].shape
    group = lax.broadcasted_iota(jnp.int32, shape, 1) // plan.window
    moved = []
    for step in range(plan.nx):
        mixed = values[step % plan.nx]
        for part in range(1, plan.nx):
            mixed = jnp.where(group == part, values[(part + step) % plan.nx], mixed)
        moved.append(pltpu.roll(mixed, step * plan.window, 1) if step else mixed)
    results = []
    for part in range(plan.nx):
        result = moved[(-part) % plan.nx]
        for other in range(1, plan.nx):
            result = jnp.where(group == other, moved[(other - part) % plan.nx], result)
        results.append(result)
    return results


def mesh_kernel(
    plan,
    group,
    grid_ref,
    x_forward_ref,
    z_table_ref,
    y_forward_ref,
    y_inverse_ref,
    line_x_ref,
    line_y_ref,
    line_z_ref,
    x_inverse_ref,
    pot_ref,
    there_out_ref,
    there_in_ref,
    back_out_ref,
    back_in_ref,
    u_ref,
    o_ref,
    mid_ref,
    send_sems,
    recv_sems,
    local_sems,
):
    parity = lax.axis_index("gz")
    device = group.me()
    row_k, nx = plan.row_k, plan.nx

    def sending(way, kind, slot, part, out_ref, in_ref):
        first, count = part
        lanes = pl.ds(first * LANES, count * LANES)
        rows = pl.ds(kind * SUBLANES, SUBLANES)
        copies = group.copies(
            lambda peer: out_ref.at[peer, rows, lanes],
            lambda place: in_ref.at[place, rows, lanes],
            lambda step: send_sems.at[way, kind, slot, step],
            lambda step: recv_sems.at[way, kind, slot, step],
        )
        own = pltpu.make_async_copy(
            out_ref.at[device, rows, lanes],
            in_ref.at[device, rows, lanes],
            local_sems.at[way, kind, slot],
        )
        return copies, own

    def start(copies, own):
        for copy in copies:
            copy.start()
        own.start()

    def arrive(copies, own):
        for copy in copies:
            copy.wait_recv()
        own.wait()

    def tile_lanes(tile):
        return pl.ds(pl.multiple_of(tile * LANES, LANES), LANES)

    def x_forward(tile, carry):
        pieces = []
        for other in range(nx):
            row = pl.multiple_of((tile * nx + other) * SUBLANES, SUBLANES)
            for octet in range(plan.octets):
                pieces.append(grid_ref[octet, pl.ds(row, SUBLANES), :])
        high, low = halves(jnp.concatenate(pieces, axis=0))
        first_pass = mm(x_forward_ref[0], jnp.concatenate([high, low], axis=0), ROWS_BY_ROWS)
        second_pass = mm(x_forward_ref[1], high, ROWS_BY_ROWS)
        total = first_pass[:, :LANES] + (first_pass[:, LANES:] + second_pass)
        there_out_ref[:, :, tile_lanes(tile)] = total.reshape(plan.dests, row_k, LANES)
        return carry

    whole = [(0, plan.tiles)]
    kinds = range(plan.groups)
    there = [
        [
            sending(0, kind, slot, part, there_out_ref, there_in_ref)
            for slot, part in enumerate(whole if kind else plan.parts)
        ]
        for kind in kinds
    ]
    back = [
        [sending(1, kind, slot, part, back_out_ref, back_in_ref) for slot, part in enumerate(plan.back_parts)]
        for kind in kinds
    ]
    for part, (first, count) in enumerate(plan.parts):
        if part == 0:
            greet([group], lambda: lax.fori_loop(first, first + count, x_forward, 0))
        else:
            lax.fori_loop(first, first + count, x_forward, 0)
        start(*there[0][part])
    for kind in kinds[1:]:
        start(*there[kind][0])

    imaginary = lax.broadcasted_iota(jnp.int32, (1, SUBLANES, 1), 1) >= plan.half_k

    def z_transform(direction, rows):
        high = z_table_ref[parity, direction, 0]
        both = jnp.concatenate([high, high], axis=0)
        low = z_table_ref[parity, direction, 1]
        total = mm(u_ref[:rows], both) + mm(u_ref[:rows, :LANES], low)
        total = total.reshape(rows // SUBLANES, SUBLANES, 2 * LANES)
        swapped = pltpu.roll(total[..., LANES:], plan.half_k, 1)
        swapped = jnp.where(imaginary == (direction == 0), -swapped, swapped)
        return (total[..., :LANES] + swapped).reshape(rows, LANES)

    def z_forward(kind, gy):
        rows = slice(kind * SUBLANES, (kind + 1) * SUBLANES)
        for tile in range(plan.tiles):
            here = pl.ds(tile * LANES, LANES)
            values = regroup(plan, [there_in_ref[gy * nx + gx, rows, here] for gx in range(nx)])
            for other in range(0, nx, 2):
                row = (tile * nx + other) * SUBLANES
                high, low = halves(jnp.concatenate(values[other : other + 2], axis=0))
                u_ref[row : row + 2 * SUBLANES, :LANES] = high
                u_ref[row : row + 2 * SUBLANES, LANES:] = low
        row = pl.multiple_of(gy * plan.rows, SUBLANES)
        mid_ref[kind, pl.ds(row, plan.rows), :] = z_transform(0, plan.rows)

    def column(kind, j):
        lines = [pl.ds(j + half * plan.half_k, plan.all_y, stride=SUBLANES) for half in range(2)]
        real = mid_ref[kind, lines[0], :]
        imag = mid_ref[kind, lines[1], :]
        stacked = jnp.concatenate(
            [jnp.concatenate([real, imag], axis=1), jnp.concatenate([imag, -real], axis=1)], axis=0
        )
        high, low = halves(stacked)
        spectrum = mm(y_forward_ref[0], high) + (mm(y_forward_ref[0], low) + mm(y_forward_ref[1], high))
        kx = device * plan.width_k + kind * plan.half_k + j
        square = (line_y_ref[0] + line_z_ref[parity, 0]) + line_x_ref[0, kx]
        factor = (line_y_ref[1] * line_z_ref[parity, 1]) * line_x_ref[1, kx]
        green = jnp.where(
            square > 0.0,
            coulomb
            * jnp.exp(square * (-np.pi**2 / (ewald * ewald * GRID * GRID)))
            * factor
            / (np.pi * GRID * jnp.maximum(square, 1.0)),
            0.0,
        )
        real = spectrum[:, :LANES] * green
        imag = spectrum[:, LANES:] * green
        stacked = jnp.concatenate(
            [jnp.concatenate([real, imag], axis=1), jnp.concatenate([-imag, real], axis=1)], axis=0
        )
        high, low = halves(stacked)
        result = mm(y_inverse_ref[0], high) + (mm(y_inverse_ref[0], low) + mm(y_inverse_ref[1], high))
        return lines, result

    def columns(kind, i):
        results = [column(kind, i * 2 + other) for other in range(2)]
        for lines, result in results:
            mid_ref[kind, lines[0], :] = result[:, :LANES]
            mid_ref[kind, lines[1], :] = result[:, LANES:]

    def z_backward(kind, part, gy):
        first, count = part
        size = count * nx * SUBLANES
        row = pl.multiple_of(gy * plan.rows + first * nx * SUBLANES, SUBLANES)
        high, low = halves(mid_ref[kind, pl.ds(row, size), :])
        u_ref[:size, :LANES] = high
        u_ref[:size, LANES:] = low
        o_ref[:size] = z_transform(1, size)
        for tile in range(count):
            values = []
            for other in range(nx):
                row = (tile * nx + other) * SUBLANES
                values.append(o_ref[row : row + SUBLANES])
            here = pl.ds((first + tile) * LANES, LANES)
            rows = slice(kind * SUBLANES, (kind + 1) * SUBLANES)
            for gx, value in enumerate(regroup(plan, values)):
                back_out_ref[gy * nx + gx, rows, here] = value

    def each(count, work, *fixed):
        def step(i, carry):
            work(*fixed, i)
            return carry

        lax.fori_loop(0, count, step, 0)

    for kind in kinds:
        for piece in there[kind]:
            arrive(*piece)
        each(plan.ny, z_forward, kind)
        each(min(plan.half_k, plan.width_k) // 2, columns, kind)
        for part, piece in zip(plan.back_parts, back[kind]):
            each(plan.ny, z_backward, kind, part)
            start(*piece)

    def x_inverse(tile, carry):
        lines = back_in_ref[:, :, tile_lanes(tile)].reshape(plan.dests * row_k, LANES)
        high, low = halves(lines.T)
        first_pass = mm(jnp.concatenate([high, low], axis=0), x_inverse_ref[0])
        value = first_pass[:LANES] + (first_pass[LANES:] + mm(high, x_inverse_ref[1]))
        lane = lax.rem(lax.broadcasted_iota(jnp.int32, value.shape, 1), plan.pack_x)
        rest = value - value.astype(jnp.bfloat16).astype(jnp.float32)
        value = jnp.where((lane >= plan.pad_x) & (lane < 2 * plan.pad_x), rest, value)
        for octet in range(plan.octets):
            for other in range(0, nx, 2):
                pieces = []
                for extra in range(2):
                    row = (other + extra) * plan.window + octet * SUBLANES
                    pieces.append(value[row : row + SUBLANES])
                row = pl.multiple_of((tile * nx + other) * SUBLANES, 2 * SUBLANES)
                pot_ref[octet, pl.ds(row, 2 * SUBLANES), :] = jnp.concatenate(pieces, axis=0).astype(jnp.bfloat16)
        return carry

    for part, (first, count) in enumerate(plan.back_parts):
        for kind in kinds:
            arrive(*back[kind][part])
        lax.fori_loop(first, first + count, x_inverse, 0)
    for pieces in there + back:
        for copies, _ in pieces:
            for copy in copies:
                copy.wait_send()


def gather_kernel(plan, counts_ref, atoms_ref, pot_ref, out_ref, list_ref, y_ref, x_ref, p_ref):
    out_ref[...] = jnp.zeros_like(out_ref)
    pack = plan.pack_x

    def work(lane, block, chunk, octet, sign):
        atoms = atoms_ref[block, :, pl.ds(pl.multiple_of(chunk * LANES, LANES), LANES)]
        weights, slopes = spline_rows(atoms[0:3])
        offset = offsets(plan.pad_x, atoms[4:5])
        table = jnp.concatenate([placed(offset, weights, 0), placed(offset, slopes, 0)], axis=1)
        high = table.astype(jnp.bfloat16).astype(jnp.float32)
        unused = jnp.zeros((pack - 3 * plan.pad_x, 2 * LANES), jnp.float32)
        x_ref[lane] = jnp.concatenate([high, high, table - high, unused], axis=0).astype(jnp.bfloat16)
        offset = offsets(plan.pad_y, atoms[5:6])
        y_ref[lane, 0] = placed(offset, weights, 1)
        y_ref[lane, 1] = placed(offset, slopes, 1)
        offset, factor = z_offsets(plan, octet, atoms[6:7])
        factor = factor * sign
        weight_z = placed(offset, weights, 2) * factor
        slope_z = placed(offset, slopes, 2) * factor
        place = pl.ds(pl.multiple_of(lax.rem(block, plan.nx) * pack, LANES), pack)
        p_ref[lane] = mm(pot_ref[octet, :, place], x_ref[lane])
        total_x = jnp.zeros((SUBLANES, LANES), jnp.float32)
        total_y = jnp.zeros((SUBLANES, LANES), jnp.float32)
        total_z = jnp.zeros((SUBLANES, LANES), jnp.float32)
        for y in range(plan.pad_y):
            rows = slice(y * SUBLANES, (y + 1) * SUBLANES)
            plain = p_ref[lane, rows, :LANES]
            weight = y_ref[lane, 0, y : y + 1]
            total_x += weight * p_ref[lane, rows, LANES:]
            total_y += y_ref[lane, 1, y : y + 1] * plain
            total_z += weight * plain
        totals = [weight_z * total_x, weight_z * total_y, slope_z * total_z]
        for dim in range(3):
            row = jnp.sum(totals[dim], axis=0, keepdims=True)
            out_ref[lax.rem(block, plan.nx), block // plan.nx, pl.ds(dim * plan.chunks + chunk, 1), :] += row

    over_units(plan, counts_ref, list_ref, work)


def vmem_call(kernel, out_shape, scratch_shapes, limit, smem=(), **params):
    def call(*operands):
        specs = [
            pl.BlockSpec(memory_space=pltpu.SMEM if i in smem else pltpu.VMEM)
            for i in range(len(operands))
        ]
        return pl.pallas_call(
            kernel,
            in_specs=specs,
            out_specs=pl.BlockSpec(memory_space=pltpu.VMEM),
            out_shape=out_shape,
            scratch_shapes=scratch_shapes,
            compiler_params=pltpu.CompilerParams(vmem_limit_bytes=limit * 2**20, **params),
        )(*operands)

    return call


def per_device(charges, fractions, base_cells, counts):
    capacity = charges.shape[0]
    plan = Plan(lax.axis_size("gz"), lax.axis_size("gy"), lax.axis_size("gx"), capacity)
    f32, bf16 = jnp.float32, jnp.bfloat16
    slot = jnp.arange(capacity, dtype=jnp.int32)
    live = slot < counts.reshape(())
    charge = jnp.where(live, charges, jnp.zeros_like(charges))
    local_x = (base_cells[0] - lax.axis_index("gx") * plan.cells_x).astype(f32)
    local_y = (base_cells[1] - lax.axis_index("gy") * plan.cells_y).astype(f32)
    key = jnp.where(live, base_cells[2] - lax.axis_index("gz") * plan.cells_z, plan.cells_z)
    key, slot, t_x, t_y, t_z, charge, local_x, local_y = lax.sort(
        [key, slot, fractions[0], fractions[1], fractions[2], charge, local_x, local_y],
        num_keys=1,
        is_stable=False,
    )
    edges = np.full(LANES, -1)
    starts = np.arange(plan.nx * plan.octets + 1) * SUBLANES
    edges[: len(starts)] = starts - plan.halo
    edges[LANES // 2 : LANES // 2 + len(starts)] = np.minimum(starts + SUBLANES, plan.cells_z)
    counted = jnp.sum((key[None, :] < jnp.asarray(edges)[:, None]).astype(f32), axis=1)
    counted = jnp.pad(counted, (0, capacity - LANES))
    atoms = jnp.stack([t_x, t_y, t_z, charge, local_x, local_y, key.astype(f32), counted])
    across, along = group_of("gz"), group_of("gx")
    most = max(plan.nz, plan.nx)
    atoms = vmem_call(
        functools.partial(atoms_kernel, across, along, plan.pieces),
        jax.ShapeDtypeStruct((plan.blocks,) + atoms.shape, f32),
        [
            pltpu.SemaphoreType.DMA((plan.nz + 1, plan.pieces, most)),
            pltpu.SemaphoreType.DMA((plan.nz + 1, plan.pieces, most)),
            pltpu.SemaphoreType.DMA,
        ],
        8,
        collective_id=0,
        has_side_effects=True,
    )(atoms)
    counts = atoms[:, 7, :LANES].astype(jnp.int32)

    lanes = plan.tiles * LANES
    mesh_shape = (plan.octets, plan.rows, plan.nx * LANES)
    units = plan.blocks * plan.chunks * plan.octets + plan.unroll
    grid = vmem_call(
        functools.partial(spread_kernel, plan),
        jax.ShapeDtypeStruct(mesh_shape, f32),
        [
            pltpu.SMEM((units,), jnp.int32),
            pltpu.VMEM((plan.unroll, plan.pad_y, LANES), f32),
            pltpu.VMEM((plan.unroll, 2 * LANES, 2 * LANES), bf16),
            pltpu.VMEM((plan.unroll, plan.rows, 2 * LANES), bf16),
        ],
        16,
        smem=(0,),
    )(counts, atoms)
    y_forward, y_inverse = plan.y_tables()
    line_x, line_y, line_z = plan.green_lines()
    group = group_of("gy", "gx")
    parts = len(plan.parts)
    half = pltpu.VMEM((plan.dests, plan.row_k, lanes), f32)
    potential = vmem_call(
        functools.partial(mesh_kernel, plan, group),
        jax.ShapeDtypeStruct((plan.octets, plan.rows, plan.nx * plan.pack_x), bf16),
        [
            half,
            half,
            half,
            half,
            pltpu.VMEM((plan.rows, 2 * LANES), bf16),
            pltpu.VMEM((plan.rows, LANES), f32),
            pltpu.VMEM((plan.groups, plan.all_y * SUBLANES, LANES), f32),
            pltpu.SemaphoreType.DMA((2, plan.groups, parts, group.count)),
            pltpu.SemaphoreType.DMA((2, plan.groups, parts, group.count)),
            pltpu.SemaphoreType.DMA((2, plan.groups, parts)),
        ],
        28,
        smem=(5,),
        collective_id=1,
        has_side_effects=True,
    )(
        grid,
        plan.x_forward(),
        plan.z_tables(),
        y_forward,
        y_inverse,
        line_x,
        line_y,
        line_z,
        plan.x_inverse(),
    )
    shares = vmem_call(
        functools.partial(gather_kernel, plan),
        jax.ShapeDtypeStruct((plan.nx, plan.nz, 3 * plan.chunks, LANES), f32),
        [
            pltpu.SMEM((units,), jnp.int32),
            pltpu.VMEM((plan.unroll, 2, plan.pad_y, LANES), f32),
            pltpu.VMEM((plan.unroll, plan.pack_x, 2 * LANES), bf16),
            pltpu.VMEM((plan.unroll, plan.rows, 2 * LANES), f32),
        ],
        16,
        smem=(0,),
    )(counts, atoms, potential)
    share = shares.shape[2:]
    return vmem_call(
        functools.partial(shares_kernel, across, along),
        jax.ShapeDtypeStruct((3, capacity), f32),
        [
            pltpu.VMEM((plan.nz,) + share, f32),
            pltpu.VMEM(shares.shape, f32),
            pltpu.VMEM((plan.nz,) + share, f32),
            pltpu.VMEM(share, f32),
            pltpu.VMEM((capacity, capacity), bf16),
            pltpu.SemaphoreType.DMA((2, most)),
            pltpu.SemaphoreType.DMA((2, most)),
        ],
        24,
        collective_id=2,
        has_side_effects=True,
    )(shares, charge.reshape(-1, LANES), slot.astype(f32).reshape(-1, LANES))


def solution(mesh):
    in_specs = (
        P(("gz", "gy", "gx")),
        P(None, ("gz", "gy", "gx")),
        P(None, ("gz", "gy", "gx")),
        P("gz", "gy", "gx"),
    )
    out_specs = P(None, ("gz", "gy", "gx"))
    return jax.shard_map(
        per_device, mesh=mesh, in_specs=in_specs, out_specs=out_specs, check_vma=False
    )
```
